32 devices in a mesh: batch: 1 (over z), sy: 4 (over y), sx: 8 (over x, core).
Axes of the slice: x: 4, y: 4, z: 1, core: 2. Of those that a mesh axis runs over, the one named last changes fastest.
The devices are a block of a 4x4x8 slice.
Arguments:
- forcing: float32 [256, 128, 192], P(('batch', 'sx'), 'sy')
- kappa: float32 [256, 128], P(('batch', 'sx'), 'sy')
- local_inv: float32 [32, 1600, 1600], P(('batch', 'sx', 'sy'))
- coarse_basis: float32 [32, 1024, 8], P(('batch', 'sx', 'sy'))
- coarse_counts: int32 [32], P(('batch', 'sx', 'sy'))
- coarse_inv: float32 [128, 128], P('batch')
Outputs:
- output 1: float32 [256, 128, 192], P(('batch', 'sx'), 'sy')
- output 2: float32 [8, 192], P('batch')
All inputs are finite; a program needn't handle non-finite values.
Results may differ from the reference program's by a relative error of at most 0.001.
Values are sent between devices in bfloat16 or wider.
A program may use at most 768 MiB of HBM per device.

```python
import jax
import jax.numpy as jnp
from jax import lax

SX = 8
SY = 4
M = 32
D = 4
KMAX = 8
B = 192
ITERS = 8
ME = M + D + D
NE = ME * ME
NPART = SX * SY
KTOT = NPART * KMAX // 2
CONTRAST = 1000.0


def edge_weights(kappa):
    kappa_pad = jnp.pad(kappa, 1, mode='edge')
    middle = kappa_pad[1:-1, 1:-1]

    def harmonic(other):
        return 2.0 * middle * other / (middle + other)
    return (harmonic(kappa_pad[:-2, 1:-1]), harmonic(kappa_pad[2:, 1:-1]), harmonic(kappa_pad[1:-1, :-2]), harmonic(kappa_pad[1:-1, 2:]))


def apply_op(weights, field):
    w_north, w_south, w_west, w_east = weights
    diagonal = w_north + w_south + w_west + w_east
    field_pad = jnp.pad(field, ((1, 1), (1, 1), (0, 0)))
    return (diagonal[:, :, None] * field - w_north[:, :, None] * field_pad[:-2, 1:-1] - w_south[:, :, None] * field_pad[2:, 1:-1] - w_west[:, :, None] * field_pad[1:-1, :-2] - w_east[:, :, None] * field_pad[1:-1, 2:])


def to_blocks(field):
    return field.reshape(SX, M, SY, M, -1).transpose(0, 2, 1, 3, 4).reshape(NPART, M * M, -1)


def from_blocks(blocks):
    return blocks.reshape(SX, SY, M, M, -1).transpose(0, 2, 1, 3, 4).reshape(SX * M, SY * M, -1)


def extend_blocks(field):
    rows = field.reshape(SX, M, SY * M, -1)
    zero_rows = jnp.zeros_like(rows[:1, :D])
    top = jnp.concatenate([zero_rows, rows[:-1, M - D:]], axis=0)
    bottom = jnp.concatenate([rows[1:, :D], zero_rows], axis=0)
    rows = jnp.concatenate([top, rows, bottom], axis=1)
    columns = rows.reshape(SX, ME, SY, M, -1)
    zero_cols = jnp.zeros_like(columns[:, :, :1, :D])
    left = jnp.concatenate([zero_cols, columns[:, :, :-1, M - D:]], axis=2)
    right = jnp.concatenate([columns[:, :, 1:, :D], zero_cols], axis=2)
    columns = jnp.concatenate([left, columns, right], axis=3)
    return columns.transpose(0, 2, 1, 3, 4)


def fold_blocks(extended):
    columns = extended.transpose(0, 2, 1, 3, 4)
    left = columns[:, :, :, :D]
    right = columns[:, :, :, M + D:]
    zero_cols = jnp.zeros_like(left[:, :, :1])
    from_right = jnp.concatenate([left[:, :, 1:], zero_cols], axis=2)
    from_left = jnp.concatenate([zero_cols, right[:, :, :-1]], axis=2)
    center = (columns[:, :, :, D:D + M] + jnp.pad(from_right, ((0, 0), (0, 0), (0, 0), (M - D, 0), (0, 0))) + jnp.pad(from_left, ((0, 0), (0, 0), (0, 0), (0, M - D), (0, 0))))
    rows = center.reshape(SX, ME, SY * M, -1)
    top = rows[:, :D]
    bottom = rows[:, M + D:]
    zero_rows = jnp.zeros_like(top[:1])
    from_below = jnp.concatenate([top[1:], zero_rows], axis=0)
    from_above = jnp.concatenate([zero_rows, bottom[:-1]], axis=0)
    center = (rows[:, D:D + M] + jnp.pad(from_below, ((0, 0), (M - D, 0), (0, 0), (0, 0))) + jnp.pad(from_above, ((0, 0), (0, M - D), (0, 0), (0, 0))))
    return center.reshape(SX * M, SY * M, -1)


def pack_order(counts):
    slot = jnp.arange(NPART * KMAX)
    valid = (slot % KMAX) < counts[slot // KMAX]
    order = jnp.argsort(jnp.where(valid, 0, 1) * (NPART * KMAX) + slot)
    return order[:KTOT]


def draw_counts(key):
    key_perm, key_shift = jax.random.split(key)
    order = jax.random.permutation(key_perm, NPART)
    shift = jax.random.randint(key_shift, (NPART // 2,), 0, KMAX // 2)
    shift = shift.at[0].set(KMAX // 2 - 1)
    counts = jnp.full((NPART,), KMAX // 2, jnp.int32)
    counts = counts.at[order[0::2]].add(shift).at[order[1::2]].add(-shift)
    return counts.astype(jnp.int32)


def build_basis(amplitude, counts):
    column = jnp.arange(KMAX)
    freq_row = (column + 1) // 2
    freq_col = column // 2
    grid = (jnp.arange(M) + 0.5) * (jnp.pi / M)
    wave_row = jnp.cos(grid[:, None] * freq_row[None, :])
    wave_col = jnp.cos(grid[:, None] * freq_col[None, :])
    modes = (wave_row[:, None, :] * wave_col[None, :, :]).reshape(M * M, KMAX)
    keep = (column[None, :] < counts[:, None]).astype(jnp.float32) * amplitude
    return modes[None, :, :] * keep[:, None, :]


def build_inverses(kappa, basis, counts):
    weights = edge_weights(kappa)
    w_north, w_south, w_west, w_east = weights
    diagonal = w_north + w_south + w_west + w_east
    east_in = w_east * (jnp.arange(SY * M) < SY * M - 1)[None, :]
    south_in = w_south * (jnp.arange(SX * M) < SX * M - 1)[:, None]
    diag_ext = extend_blocks(diagonal[:, :, None] - 1.0).reshape(NPART, ME, ME) + 1.0
    east_ext = extend_blocks(east_in[:, :, None]).reshape(NPART, ME, ME) * (jnp.arange(ME) < ME - 1)[None, None, :]
    south_ext = extend_blocks(south_in[:, :, None]).reshape(NPART, ME, ME) * (jnp.arange(ME) < ME - 1)[None, :, None]

    def local_matrix(pieces):
        diag_block, east_block, south_block = pieces
        east_flat = east_block.reshape(-1)[:-1]
        south_flat = south_block.reshape(-1)[:-ME]
        matrix = jnp.diag(diag_block.reshape(-1)) - jnp.diag(east_flat, 1) - jnp.diag(east_flat, -1) - jnp.diag(south_flat, ME) - jnp.diag(south_flat, -ME)
        return jnp.linalg.inv(matrix)
    local_inv = lax.map(local_matrix, (diag_ext, east_ext, south_ext))
    local_inv = 0.5 * (local_inv + jnp.swapaxes(local_inv, 1, 2))

    def coarse_row(index):
        single = basis * (jnp.arange(NPART) == index)[:, None, None]
        image = apply_op(weights, from_blocks(single))
        return jnp.einsum('smk,smc->skc', basis, to_blocks(image)).reshape(NPART * KMAX, KMAX)
    stacked = lax.map(coarse_row, jnp.arange(NPART))
    full = jnp.transpose(stacked, (1, 0, 2)).reshape(NPART * KMAX, NPART * KMAX)
    packed = pack_order(counts)
    coarse = full[packed][:, packed]
    coarse_inv = jnp.linalg.inv(coarse)
    coarse_inv = 0.5 * (coarse_inv + coarse_inv.T)
    return local_inv, coarse_inv


def setup_inputs(seed: int = 0, part: int = 0) -> dict:
    key = jax.random.fold_in(jax.random.key(seed), part)
    keys = jax.random.split(key, 6)
    base = jnp.exp(0.5 * jax.random.normal(keys[0], (SX * M, SY * M), jnp.float32))
    row_channel = jax.random.randint(keys[1], (SX * M,), 0, 6) == 0
    col_channel = jax.random.randint(keys[2], (SY * M,), 0, 6) == 0
    kappa = base * jnp.where(row_channel[:, None] | col_channel[None, :], CONTRAST, 1.0)
    counts = draw_counts(keys[3])
    forcing = jax.random.normal(keys[4], (SX * M, SY * M, B), jnp.float32)
    amplitude = jax.random.uniform(keys[5], (NPART, KMAX), jnp.float32, 0.5, 1.5)
    basis = build_basis(amplitude, counts)
    local_inv, coarse_inv = build_inverses(kappa, basis, counts)
    return {'forcing': forcing, 'kappa': kappa, 'local_inv': local_inv, 'coarse_basis': basis, 'coarse_counts': counts, 'coarse_inv': coarse_inv}


def reference(forcing, kappa, local_inv, coarse_basis, coarse_counts, coarse_inv):
    weights = edge_weights(kappa)
    packed = pack_order(coarse_counts)

    def col_dot(first, second):
        return jnp.sum(first * second, axis=(0, 1))

    def precondition(resid):
        extended = extend_blocks(resid).reshape(NPART, NE, B)
        local = jnp.einsum('sij,sjb->sib', local_inv.astype(jnp.float32), extended)
        level_one = fold_blocks(local.reshape(SX, SY, ME, ME, B))
        restrict = jnp.einsum('smk,smb->skb', coarse_basis, to_blocks(resid)).reshape(NPART * KMAX, B)
        coarse = jnp.dot(coarse_inv, restrict[packed])
        spread = jnp.zeros((NPART * KMAX, B), jnp.float32).at[packed].set(coarse)
        level_two = from_blocks(jnp.einsum('smk,skb->smb', coarse_basis, spread.reshape(NPART, KMAX, B)))
        return level_one + level_two

    forcing_norm = jnp.sqrt(col_dot(forcing, forcing))
    solution = jnp.zeros_like(forcing)
    resid = forcing
    precond = precondition(resid)
    direction = precond
    rz_dot = col_dot(resid, precond)
    norms = []
    for step in range(ITERS):
        image = apply_op(weights, direction)
        alpha = rz_dot / col_dot(direction, image)
        solution = solution + alpha * direction
        resid = resid - alpha * image
        norms.append(jnp.sqrt(col_dot(resid, resid)) / forcing_norm)
        if step < ITERS - 1:
            precond = precondition(resid)
            rz_new = col_dot(resid, precond)
            direction = precond + (rz_new / rz_dot) * direction
            rz_dot = rz_new
    return solution, jnp.stack(norms)
```

```python
import math
import jax
import jax.numpy as jnp
from jax import lax
from jax.experimental import pallas as pl
from jax.experimental.pallas import tpu as pltpu
from jax.sharding import PartitionSpec as P

ITERS = 8
MESH = pl.DeviceIdType.MESH
F32 = jnp.float32
BF16 = jnp.bfloat16
DIRS = (('N', -1, 0), ('S', 1, 0), ('W', 0, -1), ('E', 0, 1), ('NW', -1, -1), ('NE', -1, 1), ('SW', 1, -1), ('SE', 1, 1))
OPP = (1, 0, 3, 2, 7, 6, 5, 4)
COMBOS = ((0, 0), (0, 1), (1, 0), (0, 2), (1, 1), (2, 0))
ONE, TWO, FOUR, SUB, LANES = 1, 2, 4, 8, 128
SLOT = 3 * SUB


def repeat(count, body, by=ONE):
    def several(i, _):
        for n in range(by):
            body(i * by + n)
        return 0
    lax.fori_loop(0, count // by, several, 0)


def split3(x):
    high = x.astype(BF16)
    rest = x - high.astype(F32)
    mid = rest.astype(BF16)
    low = (rest - mid.astype(F32)).astype(BF16)
    return high, mid, low


def dot(a, b):
    return jnp.dot(a, b, preferred_element_type=F32)


def dot_highest(a, b):
    return jnp.dot(a, b, precision=lax.Precision.HIGHEST, preferred_element_type=F32)


def make_kernel(n_row, n_col, size, over, n_rhs, kmax, ktot):
    edge = size + 2 * over
    own = size * size
    strip = over * size
    corner = over * over
    ext = edge * edge
    n_dev = n_row * n_col
    lo, hi = over, over + size
    msg = strip + size + 2 * over
    cmsg = corner + 2 * over
    batch1 = 4 * msg + 4 * cmsg
    rows_all = batch1 + own
    k_main = own + 4 * strip
    k_corner = 4 * corner
    ring = size + 8
    u_off = [0, msg, 2 * msg, 3 * msg] + [4 * msg + cmsg * i for i in range(4)]
    u_len = [msg] * 4 + [cmsg] * 4
    h_off = [strip, 0, 2 * strip, 3 * strip] + [4 * strip + corner * i for i in range(4)]
    h_len = [strip] * 4 + [corner] * 4
    halves = ((0, LANES), (LANES, n_rhs))
    tail = n_rhs - LANES
    n_chip = n_dev // TWO

    def packed(rows):
        left = -(-rows // (TWO * SUB)) * SUB
        return left, rows + left
    m_len = [packed(n)[ONE] for n in u_len]
    m_off = [sum(m_len[:k]) for k in range(8)]
    q_len = [packed(n)[ONE] for n in h_len]
    q_rank = (1, 0, 2, 3, 4, 5, 6, 7)
    q_off = [sum(q_len[j] for j in range(8) if q_rank[j] < q_rank[k]) for k in range(8)]
    tiles = [(c, min(c + 128, ext)) for c in range(0, ext, 128)]
    half_own = own // 2

    def kernel(f_hbm, kappa_ref, l_hbm, basis_t_ref, count_ref, cinv_ref,
               x_ref, norm_ref,
               nat, perm, stage, lp, lc, rp, rc, v, pack, h_out, halo, u, g_out, g_raw, g, r, p, s, ms, z, mc, ag, ags, cell_ref,
               coef, bcat, b_t, c_map, edges, pack_c, ring_v, cg, nb, scal, c32,
               l_sem, f_sem, e_send, e_recv, h_send, h_recv, g_send, g_recv, ag_send, ag_recv, fw_send, fw_recv):
        row_id = lax.axis_index('sx')
        col_id = lax.axis_index('sy')
        me = row_id * n_col + col_id
        parity = row_id % TWO
        my_slot = (row_id // TWO) * n_col + col_id

        def has(k):
            _, dr, dc = DIRS[k]
            ok = True
            for pos, step, count in ((row_id, dr, n_row), (col_id, dc, n_col)):
                if step < 0:
                    test = pos > 0
                elif step > 0:
                    test = pos < count - 1
                else:
                    continue
                ok = test if ok is True else jnp.logical_and(ok, test)
            return ok

        def there(k):
            return {'sx': row_id + DIRS[k][1], 'sy': col_id + DIRS[k][2]}

        exists = [has(k) for k in range(8)]

        def remote(src, dst, send, recv, k):
            return pltpu.make_async_remote_copy(src_ref=src, dst_ref=dst, send_sem=send, recv_sem=recv, device_id=there(k), device_id_type=MESH)

        def band_copy(j):
            lines = pl.ds(over * j, over)
            return pltpu.make_async_copy(l_hbm.at[lines], nat.at[lines], l_sem.at[j])
        for j in range(edge // over):
            band_copy(j).start()
        f_copy = pltpu.make_async_copy(f_hbm, v, f_sem.at[0])
        f_copy.start()
        r_copy = pltpu.make_async_copy(f_hbm, r, f_sem.at[1])
        r_copy.start()

        for ref in (halo, g_raw, g_out, ags, p, s, ms, z, x_ref):
            ref[...] = jnp.zeros_like(ref)
        for i in range(size):
            cell_ref[size * i:size * i + size, 0:LANES] = jnp.broadcast_to(kappa_ref[i:i + ONE, :], (LANES, size)).T
        for c in range(0, own, LANES):
            cell_ref[c:c + LANES, LANES:LANES + kmax] = basis_t_ref[:, c:c + LANES].T
        for i in range(size):
            pack_c[0, i:i + 1, :] = cell_ref[size * i:size * i + 1, :]
            pack_c[1, i:i + 1, :] = cell_ref[size * i + size - 1:size * i + size, :]
        edges[0] = cell_ref[0:size, :]
        edges[1] = cell_ref[own - size:own, :]
        edges[2] = pack_c[0]
        edges[3] = pack_c[1]

        barrier = pltpu.get_barrier_semaphore()

        for d in range(ONE, n_dev):
            peer = (me + d) % n_dev
            pl.semaphore_signal(barrier, inc=ONE, device_id={'sx': peer // n_col, 'sy': peer % n_col}, device_id_type=MESH)
        pl.semaphore_wait(barrier, n_dev - 1)

        edge_src = [cell_ref.at[pl.ds(0, size)], cell_ref.at[pl.ds(own - size, size)], pack_c.at[0], pack_c.at[1]]
        edge_copy = [remote(edge_src[k], edges.at[OPP[k]], e_send.at[k], e_recv.at[OPP[k]], k) for k in range(4)]
        edge_in = [remote(edge_src[k], edges.at[k], e_send.at[k], e_recv.at[k], k) for k in range(4)]
        for k in range(4):
            @pl.when(exists[k])
            def _(k=k):
                edge_copy[k].start()

        sub8 = lax.broadcasted_iota(jnp.int32, (8, n_rhs), 0)
        low4 = sub8 < 4

        def roll4(t):
            return pltpu.roll(t, 4, 0)

        def slices(ref, off, length):
            return [ref.at[pl.ds(off[k], length[k])] for k in range(8)]
        h_src, h_dst = slices(h_out, q_off, q_len), slices(halo, q_off, q_len)
        h_copy = [remote(h_src[k], h_dst[OPP[k]], h_send.at[k], h_recv.at[OPP[k]], k) for k in range(8)]
        h_in = [remote(h_src[k], h_dst[k], h_send.at[k], h_recv.at[k], k) for k in range(8)]
        g_src, g_dst = slices(g_out, m_off, m_len), slices(g_raw, m_off, m_len)
        g_copy = [remote(g_src[k], g_dst[OPP[k]], g_send.at[k], g_recv.at[OPP[k]], k) for k in range(8)]
        g_in = [remote(g_src[k], g_dst[k], g_send.at[k], g_recv.at[k], k) for k in range(8)]

        def pack_message(out, at, src, first, rows):
            left, _ = packed(rows)
            out[at:at + rows, :] = src[first:first + rows, 0:LANES]
            at = at + rows
            out[at:at + left, 0:tail] = src[first:first + left, LANES:n_rhs]
            out[at:at + rows - left, LANES - tail:LANES] = src[first + left:first + rows, LANES:n_rhs]

        def each(copies, what):
            for k in (4, 5, 6, 7, 2, 3, 0, 1):
                @pl.when(exists[k])
                def _(k=k):
                    if what == 'start':
                        copies[k].start()
                    elif what == 'recv':
                        copies[k].wait_recv()
                    else:
                        copies[k].wait_send()

        def own_slot(par):
            return ag.at[par, 0, pl.ds(pl.multiple_of(my_slot * SLOT, SUB), SLOT)]

        def ag_start(par):
            ag[par, 0, pl.ds(pl.multiple_of(my_slot * SLOT, SUB), SLOT), :] = ags[par]
            for d in range(ONE, n_chip):
                peer = (my_slot + d) % n_chip
                pltpu.make_async_remote_copy(
                    src_ref=ags.at[par], dst_ref=own_slot(par), send_sem=ag_send.at[par], recv_sem=ag_recv.at[par],
                    device_id={'sx': TWO * (peer // n_col) + parity, 'sy': peer % n_col}, device_id_type=MESH).start()

        def ag_wait(par, sem):
            many = ag.at[par, 0, pl.ds(0, (n_chip - ONE) * SLOT)]
            pltpu.make_async_copy(many, many, sem.at[par]).wait()

        def forward(par):
            return pltpu.make_async_remote_copy(
                src_ref=ag.at[par, 0], dst_ref=ag.at[par, ONE], send_sem=fw_send.at[par], recv_sem=fw_recv.at[par],
                device_id={'sx': row_id + ONE - TWO * parity}, device_id_type=MESH)

        def ag_forward(par):
            ag_wait(par, ag_recv)
            forward(par).start()

        def ag_done(par):
            ag_wait(par, ag_send)
            forward(par).wait_send()

        def rows_sum(t):
            return jnp.sum(t, axis=0, keepdims=True)

        def pack_sides():
            for q in range(size // TWO):
                for c0, c1 in halves:
                    a, b = TWO * q * size, (TWO * q + ONE) * size
                    m = low4[:, :c1 - c0]
                    pack[0, SUB * q:SUB * q + SUB, c0:c1] = jnp.where(m, v[a:a + SUB, c0:c1], roll4(v[b:b + SUB, c0:c1]))
                    a, b = b - SUB, b + size - SUB
                    pack[ONE, SUB * q:SUB * q + SUB, c0:c1] = jnp.where(m, roll4(v[a:a + SUB, c0:c1]), v[b:b + SUB, c0:c1])
            sides = (pack.at[0], pack.at[ONE])
            for k, (src, first) in enumerate(((v, 0), (v, own - strip), (sides[0], 0), (sides[ONE], 0), (sides[0], 0), (sides[ONE], 0),
                                              (sides[0], strip - corner), (sides[ONE], strip - corner))):
                pack_message(h_out, q_off[k], src, first, h_len[k])

        f_copy.wait()
        r_copy.wait()
        pack_sides()
        each(h_copy, 'start')

        bt = split3(basis_t_ref[...])
        for i in range(3):
            c32[8 * i:8 * i + 8, :] = bt[i].astype(F32)
        b_t[...] = c32[...].astype(BF16)

        def split_own(i):
            rows = pl.ds(pl.multiple_of(i * size, size), size)
            parts = split3(v[rows, :])
            for j in range(3):
                rp[j, rows, :] = parts[j]
        repeat(size, split_own, FOUR)

        def restrict(par):
            d1 = dot(b_t[...], rp[0, 0:own, :])
            d2 = dot(b_t[0:16, :], rp[1, 0:own, :])
            d3 = dot(b_t[0:16, :], rp[2, 0:own, :])
            d = (d1[16:24] + d2[8:16] + d3[0:8]) + (d1[8:16] + d2[0:8]) + d1[0:8]
            ags[par, SUB:TWO * SUB, :] = d[:, 0:LANES]
            ags[par, TWO * SUB:SLOT, 0:tail] = d[:, LANES:n_rhs]

        restrict(0)
        ags[0, 0:ONE, :] = count_ref[0:ONE, :]
        ag_start(0)

        for k in range(4):
            @pl.when(exists[k])
            def _(k=k):
                edge_in[k].wait_recv()
                edge_copy[k].wait_send()

        def turn(count, col):
            for c0, c1 in tiles:
                turned = stage[0:count, c0:c1].T
                for n in range(c0, c1, 8):
                    perm[n // edge, n % edge:n % edge + 8, pl.ds(col, count)] = turned[n - c0:n - c0 + 8]

        def turn_band(jj):
            band_copy(jj).wait()
            for i in range(over):
                stage[size * i:size * i + size, :] = nat[over * jj + i, lo:hi, :]
            block = (jj + size // over + 1) % (size // over + 2)
            turn(strip, pl.multiple_of(block * strip, strip))
        repeat(edge // over, turn_band)
        for side, b0 in ((0, 0), (1, hi)):
            for i in range(size):
                stage[over * i:over * i + over, :] = nat[lo + i, b0:b0 + over, :]
            turn(strip, own + 2 * strip + side * strip)
        for q, (a0, b0) in enumerate(((0, 0), (0, hi), (hi, 0), (hi, hi))):
            for i in range(over):
                stage[corner * q + over * i:corner * q + over * i + over, :] = nat[a0 + i, b0:b0 + over, :]
        turn(k_corner, k_main)

        def put_parts(rows, x, xc):
            parts = split3(x)
            for j in range(3):
                lp[j, rows, :] = parts[j]
            c = [t.astype(F32) for t in split3(xc)]
            order = (c[0], c[0], c[0], c[1], c[1], c[2])
            lc[rows, :] = jnp.concatenate(order, axis=1).astype(BF16)

        def put_own(i):
            rows = pl.ds(pl.multiple_of(batch1 + i * size, size), size)
            put_parts(rows, perm[lo + i, lo:hi, 0:k_main], perm[lo + i, lo:hi, k_main:ext])
        repeat(size, put_own)

        def take(at, a0, na, b0, nb_):
            for i in range(na):
                stage[at + nb_ * i:at + nb_ * i + nb_, :] = perm[a0 + i, b0:b0 + nb_, :]
            return at + na * nb_

        def take_col(at, a0, na, b):
            for i in range(na):
                stage[at + i:at + i + 1, :] = perm[a0 + i, b:b + 1, :]
            return at + na

        def flush(count, first):
            step = 48

            def go(i):
                src = pl.ds(pl.multiple_of(i * step, step), step)
                dst = pl.ds(pl.multiple_of(first + i * step, step), step)
                put_parts(dst, stage[src, 0:k_main], stage[src, k_main:ext])
            repeat(count // step, go)

        at = 0
        for a_strip, a_own in ((0, lo), (hi, hi - 1)):
            at = take(at, a_strip, over, lo, size)
            at = take(at, a_own, 1, lo, size)
            at = take_col(at, a_strip, over, lo - 1)
            at = take_col(at, a_strip, over, hi)
        flush(at, 0)
        at = 0
        for b_strip, b_own in ((0, lo), (hi, hi - 1)):
            at = take(at, lo, size, b_strip, over)
            at = take_col(at, lo, size, b_own)
            at = take(at, lo - 1, 1, b_strip, over)
            at = take(at, hi, 1, b_strip, over)
        flush(at, 2 * msg)
        at = 0
        for a_strip, a_own in ((0, lo), (hi, hi - 1)):
            for b_strip, b_own in ((0, lo), (hi, hi - 1)):
                at = take(at, a_strip, over, b_strip, over)
                at = take(at, a_own, 1, b_strip, over)
                at = take_col(at, a_strip, over, b_own)
        flush(at, 4 * msg)

        k5 = 5 * kmax

        def put_basis(i, first, x):
            parts = [t.astype(F32) for t in split3(x)]
            perm[i, 0:size, 0:256] = jnp.zeros((size, 256), F32)
            for c, (j, _) in enumerate(COMBOS):
                perm[i, 0:size, k5 * c + first:k5 * c + first + kmax] = parts[j]
            bcat[pl.ds(pl.multiple_of(i * size, size), size), :] = perm[i, 0:size, 0:256].astype(BF16)

        def put_basis_line(i):
            put_basis(i, 0, cell_ref[pl.ds(pl.multiple_of(i * size, size), size), LANES:LANES + kmax])
        repeat(size, put_basis_line, TWO)
        for k in range(4):
            put_basis(size + k, kmax * (k + 1), edges[k, :, LANES:LANES + kmax])
        coef[...] = jnp.zeros_like(coef)

        width = LANES
        sub_k = lax.broadcasted_iota(jnp.int32, (8, width), 0)
        for i in range(size):
            perm[i, 0:size, 0:width] = cell_ref[size * i:size * i + size, 0:width]
            perm[i, size:ring, 0:width] = jnp.where(sub_k == 0, edges[3, i:i + 1, 0:width], edges[2, i:i + 1, 0:width])
        perm[size, 0:size, 0:width] = edges[1, :, 0:width]
        perm[size + 1, 0:size, 0:width] = edges[0, :, 0:width]
        wn, ws, ww, we, wd = range(5)

        def harmonic(a, b):
            return 2.0 * a * b / (a + b)

        def put_weights(i):
            rows = pl.ds(pl.multiple_of(i * size, size), size)
            mid = perm[i, 0:ring, 0:width]
            up = perm[(i + size + 1) % (size + 2), 0:size, 0:width]
            down = perm[i + 1, 0:size, 0:width]
            here = mid[0:size]
            a = harmonic(here, up)
            b = harmonic(here, down)
            c = harmonic(here, pltpu.roll(mid, 1, 0)[0:size])
            d = harmonic(here, pltpu.roll(mid, ring - 1, 0)[0:size])
            scal[wn, rows, :] = a
            scal[ws, rows, :] = b
            scal[ww, rows, :] = c
            scal[we, rows, :] = d
            scal[wd, rows, :] = a + b + c + d
        repeat(size, put_weights, FOUR)

        ag_forward(0)
        forward(0).wait_recv()
        n_slot = n_dev * SLOT
        dev_rows = ag[0].reshape(n_dev, SLOT, LANES)[:, 0:ONE, 0:SUB]
        count_row = jnp.broadcast_to(dev_rows, (n_dev, SLOT, SUB)).reshape(n_slot, SUB).T
        count_dev = jnp.broadcast_to(dev_rows, (n_dev, SUB, SUB)).reshape(n_dev * SUB, SUB).T

        def floor_div(a, b):
            return jnp.floor((a + 0.5) * (ONE / b))

        def slot_facts(shape, axis, step=ONE):
            at = lax.broadcasted_iota(jnp.int32, shape, axis).astype(F32) * float(step)
            slot = floor_div(at, SLOT)
            inside = at - slot * SLOT
            other = floor_div(slot, n_chip)
            chip = slot - other * n_chip
            line = floor_div(chip, n_col)
            mine = parity.astype(F32)
            odd = mine + other - TWO * mine * other
            return (TWO * line + odd) * n_col + (chip - line * n_col), inside
        sub_r, inside_r = slot_facts((n_dev * SUB, n_slot), 0, SLOT // SUB)
        sub_c, _ = slot_facts((n_dev * SUB, n_slot), ONE)
        before = jnp.where(jnp.logical_and(inside_r == 0.0, sub_r < sub_c), 1.0, 0.0).astype(F32)
        start_row = dot_highest(count_dev, before)
        _, place = slot_facts((SUB, n_slot), ONE)
        which = lax.broadcasted_iota(jnp.int32, (ktot, n_slot), 0).astype(F32)

        def one_hot(first):
            here = place - first
            target = jnp.where(jnp.logical_and(here >= 0.0, here < count_row), start_row + here, -1.0)
            return jnp.where(which == target[0:ONE, :], 1.0, 0.0).astype(F32)
        pack_low, pack_high = one_hot(SUB), one_hot(TWO * SUB)
        k_row = lax.broadcasted_iota(jnp.int32, (k5, n_slot), 0).astype(F32)
        block = floor_div(k_row, kmax)
        sub_k, inside_k = slot_facts((k5, n_slot), ONE)
        wanted = me.astype(F32) + jnp.zeros((k5, n_slot), F32)
        present = block == 0.0
        for k in range(4):
            shift = DIRS[k][1] * n_col + DIRS[k][2]
            wanted = wanted + jnp.where(block == k + ONE, float(shift), 0.0)
            present = jnp.logical_or(present, jnp.logical_and(block == k + ONE, exists[k]))
        chosen = jnp.logical_and(sub_k == wanted, inside_k == SUB + k_row - block * kmax)
        select = jnp.where(jnp.logical_and(chosen, present), 1.0, 0.0).astype(F32)
        pick = lax.dot_general(select, pack_low, (((1,), (1,)), ((), ())), precision=lax.Precision.HIGHEST, preferred_element_type=F32)
        pick = dot_highest(pick, cinv_ref[...])
        c_map[0:k5, :] = dot_highest(pick, pack_low)
        c_map[k5:TWO * k5, :] = dot_highest(pick, pack_high)

        def field(par):
            for h, (c0, c1) in enumerate(halves):
                w_ = c1 - c0

                def line(i, sums):
                    rows = pl.ds(pl.multiple_of(i * size, size), size)
                    mid = z[i, :, c0:c1]
                    here = mid[0:size]
                    up = z[(i + size + ONE) % (size + TWO), 0:size, c0:c1]
                    down = z[i + ONE, 0:size, c0:c1]
                    left = pltpu.roll(mid, ONE, 0)[0:size]
                    right = pltpu.roll(mid, ring - ONE, 0)[0:size]
                    out = (scal[wd, rows, 0:w_] * here - scal[wn, rows, 0:w_] * up - scal[ws, rows, 0:w_] * down
                           - scal[ww, rows, 0:w_] * left - scal[we, rows, 0:w_] * right)
                    v[rows, c0:c1] = out
                    parts = split3(out)
                    for j in range(3):
                        rp[j, rows, c0:c1] = parts[j]
                    res = r[rows, c0:c1]
                    new = []
                    for total, t in zip(sums, (res * here, here * out, here * s[rows, c0:c1], res * res)):
                        q = t[0:SUB]
                        for n in range(SUB, size, SUB):
                            q = q + t[n:n + SUB]
                        new.append(total + q)
                    return tuple(new)

                def lines(i, sums):
                    for n in range(FOUR):
                        sums = line(i * FOUR + n, sums)
                    return sums
                sums = lax.fori_loop(0, size // FOUR, lines, tuple(jnp.zeros((SUB, w_), F32) for _ in range(FOUR)))
                for n in range(FOUR):
                    ags[par, FOUR * h + n:FOUR * h + n + ONE, 0:w_] = rows_sum(sums[n])

        def totals(par):
            return jnp.sum(ag[par].reshape(n_dev, SLOT, LANES)[:, 0:SUB, :], axis=0)

        def products(rows, k0, k1):
            out = None
            for i, j in COMBOS:
                t = dot(lp[i, rows, k0:k1], rp[j, k0:k1, :])
                out = t if out is None else out + t
            return out

        def scalars(par, it):
            t = totals(par)
            for h, (c0, c1) in enumerate(halves):
                rz, zw, zs, rr = [t[FOUR * h + n:FOUR * h + n + ONE, 0:c1 - c0] for n in range(FOUR)]
                nb[it, :, c0:c1] = jnp.broadcast_to(rr, (SUB, c1 - c0))
                old_rz, old_pq = cg[0, 0:ONE, c0:c1], cg[ONE, 0:ONE, c0:c1]
                first = it <= ONE
                beta = jnp.where(first, 0.0, rz / old_rz)
                pq = zw + jnp.where(first, 0.0, 2.0 * beta * zs + beta * beta * old_pq)
                for n, value in enumerate((rz, pq, rz / pq, beta)):
                    cg[n, 0:ONE, c0:c1] = value

        def advance():
            for c0, c1 in halves:
                alpha = cg[TWO, 0:ONE, c0:c1]
                beta = cg[3, 0:ONE, c0:c1]

                def line(i):
                    rows = pl.ds(pl.multiple_of(i * size, size), size)
                    new_p = z[i, 0:size, c0:c1] + beta * p[rows, c0:c1]
                    new_s = v[rows, c0:c1] + beta * s[rows, c0:c1]
                    p[rows, c0:c1] = new_p
                    s[rows, c0:c1] = new_s
                    x_ref[rows, c0:c1] = x_ref[rows, c0:c1] + alpha * new_p
                    r[rows, c0:c1] = r[rows, c0:c1] - alpha * new_s
                repeat(size, line, TWO)

        gn, gs, gw, ge, gnw, gne, gsw, gse = u_off

        def fold():
            mine = batch1
            for k in range(8):
                first, rows, at = u_off[k], u_len[k], m_off[k]
                left, _ = packed(rows)
                g[first:first + rows, 0:LANES] = g_raw[at:at + rows, :]
                at = at + rows
                g[first:first + left, LANES:n_rhs] = g_raw[at:at + left, 0:tail]
                g[first + left:first + rows, LANES:n_rhs] = g_raw[at:at + rows - left, LANES - tail:LANES]
            u[mine:mine + strip, :] = u[mine:mine + strip, :] + g[gn:gn + strip, :]
            u[mine + own - strip:mine + own, :] = u[mine + own - strip:mine + own, :] + g[gs:gs + strip, :]
            for side, first, last in ((gw, gnw, gsw), (ge, gne, gse)):
                g[side:side + corner, :] = g[side:side + corner, :] + g[first:first + corner, :]
                end = side + strip
                g[end - corner:end, :] = g[end - corner:end, :] + g[last:last + corner, :]

            def last_rows(k):
                first = u_off[k] + u_len[k] - 8
                return g[first:first + 8, :]
            t = [last_rows(k) for k in range(8)]
            n_, s_, w_, e_, nw, ne, sw, se = t

            def lower(a):
                return jnp.where(low4, a, 0.0)

            def upper(a):
                return jnp.where(low4, 0.0, a)

            edge_sum = [
                (g[gn + strip:gn + strip + size, :] + u[gn + strip - size:gn + strip, :], lower(w_ + nw), upper(roll4(e_) + roll4(ne))),
                (g[gs + strip:gs + strip + size, :] + u[gs:gs + size, :], lower(roll4(w_) + sw), upper(e_ + roll4(se))),
                (g[gw + strip:gw + strip + size, :], lower(n_ + roll4(nw)), upper(roll4(s_) + sw)),
                (g[ge + strip:ge + strip + size, :], lower(roll4(n_) + roll4(ne)), upper(s_ + se)),
            ]
            for k in range(4):
                base, first, last = edge_sum[k]
                ring_v[k] = base + mc[own + size * k:own + size * k + size, :]
                ring_v[k, 0:8, :] = ring_v[k, 0:8, :] + first
                ring_v[k, size - 8:size, :] = ring_v[k, size - 8:size, :] + last

            for c0, c1 in halves:
                w = c1 - c0
                alpha = cg[TWO, 0:ONE, c0:c1]
                beta = cg[3, 0:ONE, c0:c1]
                sub = sub8[:, :w]
                low = low4[:, :w]
                at_w = jnp.logical_and(sub == 7, exists[2])
                at_e = jnp.logical_and(sub == 0, exists[3])

                def push(i, a, b, m):
                    new = m + beta * ms[i, a:b, c0:c1]
                    ms[i, a:b, c0:c1] = new
                    z[i, a:b, c0:c1] = z[i, a:b, c0:c1] - alpha * new

                def eight_lines(b):
                    tile = pl.ds(pl.multiple_of(8 * b, 8), 8)
                    ring_w = ring_v[2, tile, c0:c1]
                    ring_e = ring_v[3, tile, c0:c1]
                    for line in range(8):
                        i = 8 * b + line
                        odd = line % 2
                        four = 4 * (i - odd)
                        if not odd:
                            tw = g[pl.ds(pl.multiple_of(gw + four, 8), 8), c0:c1]
                            te = g[pl.ds(pl.multiple_of(ge + four, 8), 8), c0:c1]
                            uw = u[pl.ds(pl.multiple_of(gw + four, 8), 8), c0:c1]
                            ue = u[pl.ds(pl.multiple_of(ge + four, 8), 8), c0:c1]
                        base = pl.multiple_of(i * size, size)
                        add_w = jnp.where(low, roll4(tw) if odd else tw, 0.0)
                        add_e = jnp.where(low, 0.0, te if odd else roll4(te))
                        for n in range(0, size, 8):
                            m = u[pl.ds(mine + base + n, 8), c0:c1] + mc[pl.ds(base + n, 8), c0:c1]
                            if n == 0:
                                m = m + add_w
                            if n == size - 8:
                                m = m + add_e
                            push(i, n, n + 8, m)
                        own_w = (uw if odd else roll4(uw)) + ring_w[line:line + 1]
                        own_e = (roll4(ue) if odd else ue) + ring_e[line:line + 1]
                        push(i, size, ring, jnp.where(at_w, own_w, jnp.where(at_e, own_e, 0.0)))
                repeat(size // SUB, eight_lines)
                push(size, 0, size, jnp.where(exists[1], ring_v[1, :, c0:c1], 0.0))
                push(size + 1, 0, size, jnp.where(exists[0], ring_v[0, :, c0:c1], 0.0))

        cg[...] = jnp.zeros_like(cg)
        first_rows = pl.ds(0, batch1)
        part_a = pl.ds(batch1, half_own)
        part_b = pl.ds(batch1 + half_own, half_own)

        def iteration(it):
            par = it % 2

            @pl.when(it > 0)
            def _():
                field(par)
                pack_sides()
                each(h_copy, 'start')
                restrict(par)
                ag_start(par)

            u[first_rows, :] = products(first_rows, 0, own)
            u[part_a, :] = products(part_a, 0, own)
            each(h_in, 'recv')
            for k in range(8):
                rows, at = h_len[k], q_off[k]
                left, _ = packed(rows)
                upper = halo[at + rows:at + rows + left, :]
                low_parts = split3(halo[at:at + rows, :])
                high_parts = split3(jnp.concatenate([upper[:, 0:tail], upper[:, tail:LANES]], axis=0))
                if k < FOUR:
                    for j in range(3):
                        rp[j, own + h_off[k]:own + h_off[k] + rows, 0:LANES] = low_parts[j]
                        rp[j, own + h_off[k]:own + h_off[k] + rows, LANES:n_rhs] = high_parts[j]
                else:
                    for n, (_, j) in enumerate(COMBOS_C):
                        first = k_corner * n + h_off[k] - FOUR * strip
                        rc[first:first + rows, 0:LANES] = low_parts[j]
                        rc[first:first + rows, LANES:n_rhs] = high_parts[j]
            u[first_rows, :] = u[first_rows, :] + (products(first_rows, own, k_main) + dot(lc[first_rows, :], rc[...]))
            for k in range(8):
                pack_message(g_out, m_off[k], u, u_off[k], u_len[k])
            each(g_copy, 'start')
            u[part_a, :] = u[part_a, :] + (products(part_a, own, k_main) + dot(lc[part_a, :], rc[...]))

            @pl.when(it > 0)
            def _():
                ag_forward(par)
            u[part_b, :] = products(part_b, 0, k_main) + dot(lc[part_b, :], rc[...])

            @pl.when(it > 0)
            def _():
                forward(par).wait_recv()
                scalars(par, it)
                advance()

            @pl.when(it == 0)
            def _():
                cg[TWO, 0:ONE, :] = jnp.full((ONE, n_rhs), -1.0, F32)

            c = dot_highest(c_map[...], ag[par].reshape(n_slot, LANES))
            for (c0, c1), value in zip(halves, (c[0:k5], c[k5:TWO * k5, 0:tail])):
                parts = split3(value)
                for n, (_, j) in enumerate(COMBOS):
                    coef[k5 * n:k5 * n + k5, c0:c1] = parts[j].astype(F32)
            mc[...] = dot(bcat[...], coef[...].astype(BF16))
            each(g_in, 'recv')
            fold()
            each(h_copy, 'sent')
            each(g_copy, 'sent')
            ag_done(par)
        repeat(ITERS, iteration)

        this, last = ITERS % TWO, (ITERS + ONE) % TWO
        field(this)
        ag_start(this)
        ag_forward(this)
        forward(this).wait_recv()
        scalars(this, ITERS)
        advance()
        for h, (c0, c1) in enumerate(halves):
            def line(i, total):
                res = r[pl.ds(pl.multiple_of(i * size, size), size), c0:c1]
                t = res * res
                for n in range(0, size, SUB):
                    total = total + t[n:n + SUB]
                return total
            total = lax.fori_loop(0, size, line, jnp.zeros((SUB, c1 - c0), F32))
            ags[last, FOUR * h + 3:FOUR * h + FOUR, 0:c1 - c0] = rows_sum(total)
        ag_start(last)
        ag_forward(last)
        forward(last).wait_recv()
        t = totals(last)
        for h, (c0, c1) in enumerate(halves):
            nb[ITERS + ONE, :, c0:c1] = jnp.broadcast_to(t[FOUR * h + 3:FOUR * h + FOUR, 0:c1 - c0], (SUB, c1 - c0))
        base_norm = jnp.sqrt(nb[ONE])
        for k in range(ITERS):
            norm_ref[k:k + ONE, :] = (jnp.sqrt(nb[k + TWO]) / base_norm)[0:ONE]
        ag_done(this)
        ag_done(last)

    COMBOS_C = ((0, 0), (0, 1), (0, 2), (1, 0), (1, 1), (2, 0))
    scratch = [
        pltpu.VMEM((edge, edge, ext), F32),
        pltpu.VMEM((edge, edge, ext), F32),
        pltpu.VMEM((2 * msg, ext), F32),
        pltpu.VMEM((3, rows_all, k_main), BF16),
        pltpu.VMEM((rows_all, 6 * k_corner), BF16),
        pltpu.VMEM((3, k_main, n_rhs), BF16),
        pltpu.VMEM((6 * k_corner, n_rhs), BF16),
        pltpu.VMEM((own, n_rhs), F32),
        pltpu.VMEM((2, strip, n_rhs), F32),
        pltpu.VMEM((sum(q_len), LANES), F32),
        pltpu.VMEM((sum(q_len), LANES), F32),
        pltpu.VMEM((rows_all, n_rhs), F32),
        pltpu.VMEM((sum(m_len), LANES), F32),
        pltpu.VMEM((sum(m_len), LANES), F32),
        pltpu.VMEM((batch1, n_rhs), F32),
        pltpu.VMEM((own, n_rhs), F32),
        pltpu.VMEM((own, n_rhs), F32),
        pltpu.VMEM((own, n_rhs), F32),
        pltpu.VMEM((size + 2, ring, n_rhs), F32),
        pltpu.VMEM((size + 2, ring, n_rhs), F32),
        pltpu.VMEM((own + 4 * size, n_rhs), F32),
        pltpu.VMEM((TWO, TWO, n_chip * SLOT, LANES), F32),
        pltpu.VMEM((TWO, SLOT, LANES), F32),
        pltpu.VMEM((own, TWO * LANES), F32),
        pltpu.VMEM((256, n_rhs), F32),
        pltpu.VMEM((own + 4 * size, 256), BF16),
        pltpu.VMEM((3 * kmax, own), BF16),
        pltpu.VMEM((10 * kmax, n_dev * SLOT), F32),
        pltpu.VMEM((4, size, 256), F32),
        pltpu.VMEM((2, size, 256), F32),
        pltpu.VMEM((4, size, n_rhs), F32),
        pltpu.VMEM((4, SUB, n_rhs), F32),
        pltpu.VMEM((ITERS + 2, 8, n_rhs), F32),
        pltpu.VMEM((5, own, 128), F32),
        pltpu.VMEM((3 * kmax, own), F32),
        pltpu.SemaphoreType.DMA((edge // over,)),
        pltpu.SemaphoreType.DMA((2,)),
        pltpu.SemaphoreType.DMA((4,)), pltpu.SemaphoreType.DMA((4,)),
        pltpu.SemaphoreType.DMA((8,)), pltpu.SemaphoreType.DMA((8,)),
        pltpu.SemaphoreType.DMA((8,)), pltpu.SemaphoreType.DMA((8,)),
    ] + [pltpu.SemaphoreType.DMA((TWO,))] * 4

    return kernel, scratch


def solution(mesh):
    n_row = mesh.shape['sx']
    n_col = mesh.shape['sy']

    def body(forcing, kappa, local_inv, coarse_basis, coarse_counts, coarse_inv):
        size = forcing.shape[0]
        n_rhs = forcing.shape[2]
        edge = math.isqrt(local_inv.shape[1])
        over = (edge - size) // 2
        kmax = coarse_basis.shape[2]
        ktot = coarse_inv.shape[0]
        own = size * size
        count = jnp.broadcast_to(coarse_counts.astype(F32)[:, None], (SUB, LANES))
        kernel, scratch = make_kernel(n_row, n_col, size, over, n_rhs, kmax, ktot)
        vmem = pl.BlockSpec(memory_space=pltpu.VMEM)
        hbm = pl.BlockSpec(memory_space=pl.ANY)
        solved, norms = pl.pallas_call(
            kernel,
            out_shape=(jax.ShapeDtypeStruct((own, n_rhs), F32), jax.ShapeDtypeStruct((ITERS, n_rhs), F32)),
            in_specs=[hbm, vmem, hbm, vmem, vmem, vmem],
            out_specs=(vmem, vmem),
            scratch_shapes=scratch,
            compiler_params=pltpu.CompilerParams(collective_id=0, has_side_effects=True, vmem_limit_bytes=67043328),
        )(forcing.reshape(own, n_rhs), kappa, local_inv.reshape(edge, edge, edge * edge), coarse_basis[0].T, count, coarse_inv)
        return solved.reshape(size, size, n_rhs), norms

    cell_spec = P(('batch', 'sx'), 'sy', None)
    sub_spec = P(('batch', 'sx', 'sy'), None, None)
    return jax.shard_map(body, mesh=mesh, in_specs=(cell_spec, P(('batch', 'sx'), 'sy'), sub_spec, sub_spec, P(('batch', 'sx', 'sy')), P('batch', None)), out_specs=(cell_spec, P('batch', None)), check_vma=False)
```

```python
import math
import jax
import jax.numpy as jnp
from jax import lax
from jax.experimental import pallas as pl
from jax.experimental.pallas import tpu as pltpu
from jax.sharding import PartitionSpec as P

ITERS = 8
MESH = pl.DeviceIdType.MESH
F32 = jnp.float32
BF16 = jnp.bfloat16
DIRS = (('N', -1, 0), ('S', 1, 0), ('W', 0, -1), ('E', 0, 1), ('NW', -1, -1), ('NE', -1, 1), ('SW', 1, -1), ('SE', 1, 1))
OPP = (1, 0, 3, 2, 7, 6, 5, 4)
COMBOS = ((0, 0), (0, 1), (1, 0), (0, 2), (1, 1), (2, 0))
ONE, TWO, FOUR, SUB, LANES = 1, 2, 4, 8, 128
SLOT = 3 * SUB


def repeat(count, body, by=ONE):
    def several(i, _):
        for n in range(by):
            body(i * by + n)
        return 0
    lax.fori_loop(0, count // by, several, 0)


def split3(x):
    high = x.astype(BF16)
    rest = x - high.astype(F32)
    mid = rest.astype(BF16)
    low = (rest - mid.astype(F32)).astype(BF16)
    return high, mid, low


def dot(a, b):
    return jnp.dot(a, b, preferred_element_type=F32)


def dot_highest(a, b):
    return jnp.dot(a, b, precision=lax.Precision.HIGHEST, preferred_element_type=F32)


def make_kernel(n_row, n_col, size, over, n_rhs, kmax, ktot):
    edge = size + 2 * over
    own = size * size
    strip = over * size
    corner = over * over
    ext = edge * edge
    n_dev = n_row * n_col
    lo, hi = over, over + size
    msg = strip + size + 2 * over
    cmsg = corner + 2 * over
    batch1 = 4 * msg + 4 * cmsg
    rows_all = batch1 + own
    k_main = own + 4 * strip
    k_corner = 4 * corner
    ring = size + 8
    u_off = [0, msg, 2 * msg, 3 * msg] + [4 * msg + cmsg * i for i in range(4)]
    u_len = [msg] * 4 + [cmsg] * 4
    h_off = [strip, 0, 2 * strip, 3 * strip] + [4 * strip + corner * i for i in range(4)]
    h_len = [strip] * 4 + [corner] * 4
    halves = ((0, LANES), (LANES, n_rhs))
    tail = n_rhs - LANES
    n_chip = n_dev // TWO

    def packed(rows):
        left = -(-rows // (TWO * SUB)) * SUB
        return left, rows + left
    m_len = [packed(n)[ONE] for n in u_len]
    m_off = [sum(m_len[:k]) for k in range(8)]
    q_len = [packed(n)[ONE] for n in h_len]
    q_rank = (1, 0, 2, 3, 4, 5, 6, 7)
    q_off = [sum(q_len[j] for j in range(8) if q_rank[j] < q_rank[k]) for k in range(8)]
    tiles = [(c, min(c + 128, ext)) for c in range(0, ext, 128)]
    half_own = own // 2

    def kernel(f_hbm, kappa_ref, l_hbm, basis_t_ref, count_ref, cinv_ref,
               x_ref, norm_ref,
               nat, perm, stage, lp, lc, rp, rc, v, pack, h_out, halo, u, g_out, g_raw, g, r, p, s, ms, z, mc, ag, ags, cell_ref,
               coef, bcat, b_t, c_map, edges, pack_c, ring_v, cg, nb, scal,
               l_sem, f_sem, e_send, e_recv, h_send, h_recv, g_send, g_recv, ag_send, ag_recv, up_send, up_recv, fw_send, fw_recv):
        row_id = lax.axis_index('sx')
        col_id = lax.axis_index('sy')
        me = row_id * n_col + col_id
        parity = row_id % TWO
        my_slot = (row_id // TWO) * n_col + col_id

        def has(k):
            _, dr, dc = DIRS[k]
            ok = True
            for pos, step, count in ((row_id, dr, n_row), (col_id, dc, n_col)):
                if step < 0:
                    test = pos > 0
                elif step > 0:
                    test = pos < count - 1
                else:
                    continue
                ok = test if ok is True else jnp.logical_and(ok, test)
            return ok

        def there(k):
            return {'sx': row_id + DIRS[k][1], 'sy': col_id + DIRS[k][2]}

        exists = [has(k) for k in range(8)]

        def remote(src, dst, send, recv, k):
            return pltpu.make_async_remote_copy(src_ref=src, dst_ref=dst, send_sem=send, recv_sem=recv, device_id=there(k), device_id_type=MESH)

        def band_copy(j):
            lines = pl.ds(over * j, over)
            return pltpu.make_async_copy(l_hbm.at[lines], nat.at[lines], l_sem.at[j])
        for j in range(edge // over):
            band_copy(j).start()
        f_copy = pltpu.make_async_copy(f_hbm, v, f_sem.at[0])
        f_copy.start()
        r_copy = pltpu.make_async_copy(f_hbm, r, f_sem.at[1])
        r_copy.start()

        for ref in (halo, g_raw, g_out, ags, p, s, ms, z, x_ref):
            ref[...] = jnp.zeros_like(ref)
        eye = lax.broadcasted_iota(jnp.int32, (size, size), 0) == lax.broadcasted_iota(jnp.int32, (size, size), ONE)
        for i in range(size):
            diagonal = jnp.where(eye, kappa_ref[i:i + ONE, :], 0.0)
            cell_ref[size * i:size * i + size, 0:LANES] = jnp.broadcast_to(jnp.sum(diagonal, axis=ONE, keepdims=True), (size, LANES))
        for c in range(0, own, LANES):
            cell_ref[c:c + LANES, LANES:LANES + kmax] = basis_t_ref[:, c:c + LANES].T
        for i in range(size):
            pack_c[0, i:i + 1, :] = cell_ref[size * i:size * i + 1, :]
            pack_c[1, i:i + 1, :] = cell_ref[size * i + size - 1:size * i + size, :]
        edges[0] = cell_ref[0:size, :]
        edges[1] = cell_ref[own - size:own, :]
        edges[2] = pack_c[0]
        edges[3] = pack_c[1]

        barrier = pltpu.get_barrier_semaphore()

        for d in range(ONE, n_dev):
            peer = (me + d) % n_dev
            pl.semaphore_signal(barrier, inc=ONE, device_id={'sx': peer // n_col, 'sy': peer % n_col}, device_id_type=MESH)
        pl.semaphore_wait(barrier, n_dev - 1)

        edge_src = [cell_ref.at[pl.ds(0, size)], cell_ref.at[pl.ds(own - size, size)], pack_c.at[0], pack_c.at[1]]
        edge_copy = [remote(edge_src[k], edges.at[OPP[k]], e_send.at[k], e_recv.at[OPP[k]], k) for k in range(4)]
        edge_in = [remote(edge_src[k], edges.at[k], e_send.at[k], e_recv.at[k], k) for k in range(4)]
        for k in range(4):
            @pl.when(exists[k])
            def _(k=k):
                edge_copy[k].start()

        sub8 = lax.broadcasted_iota(jnp.int32, (8, n_rhs), 0)
        low4 = sub8 < 4

        def roll4(t):
            return pltpu.roll(t, 4, 0)

        def slices(ref, off, length):
            return [ref.at[pl.ds(off[k], length[k])] for k in range(8)]
        h_src, h_dst = slices(h_out, q_off, q_len), slices(halo, q_off, q_len)
        h_copy = [remote(h_src[k], h_dst[OPP[k]], h_send.at[k], h_recv.at[OPP[k]], k) for k in range(8)]
        h_in = [remote(h_src[k], h_dst[k], h_send.at[k], h_recv.at[k], k) for k in range(8)]
        g_src, g_dst = slices(g_out, m_off, m_len), slices(g_raw, m_off, m_len)
        g_copy = [remote(g_src[k], g_dst[OPP[k]], g_send.at[k], g_recv.at[OPP[k]], k) for k in range(8)]
        g_in = [remote(g_src[k], g_dst[k], g_send.at[k], g_recv.at[k], k) for k in range(8)]

        def pack_message(out, at, src, first, rows):
            left, _ = packed(rows)
            out[at:at + rows, :] = src[first:first + rows, 0:LANES]
            at = at + rows
            out[at:at + left, 0:tail] = src[first:first + left, LANES:n_rhs]
            out[at:at + rows - left, LANES - tail:LANES] = src[first + left:first + rows, LANES:n_rhs]

        def each(copies, what):
            for k in (2, 3, 0, 1, 4, 5, 6, 7):
                @pl.when(exists[k])
                def _(k=k):
                    if what == 'start':
                        copies[k].start()
                    elif what == 'recv':
                        copies[k].wait_recv()
                    else:
                        copies[k].wait_send()

        def own_slot(par):
            return ag.at[par, 0, pl.ds(pl.multiple_of(my_slot * SLOT, SUB), SLOT)]

        def ag_start(par):
            ag[par, 0, pl.ds(pl.multiple_of(my_slot * SLOT, SUB), SLOT), :] = ags[par]
            for d in range(ONE, n_col):
                pltpu.make_async_remote_copy(
                    src_ref=ags.at[par], dst_ref=own_slot(par), send_sem=ag_send.at[par], recv_sem=ag_recv.at[par],
                    device_id={'sy': (col_id + d) % n_col}, device_id_type=MESH).start()

        def waits(par, sem, slots):
            many = ag.at[par, 0, pl.ds(0, slots * SLOT)]
            pltpu.make_async_copy(many, many, sem.at[par]).wait()

        def ag_second(par):
            waits(par, ag_recv, n_col - ONE)
            line = ag.at[par, 0, pl.ds(pl.multiple_of((row_id // TWO) * (n_col * SLOT), SUB), n_col * SLOT)]
            for d in range(ONE, n_row // TWO):
                pltpu.make_async_remote_copy(
                    src_ref=line, dst_ref=line, send_sem=up_send.at[par], recv_sem=up_recv.at[par],
                    device_id={'sx': (row_id + TWO * d) % n_row}, device_id_type=MESH).start()

        def forward(par):
            return pltpu.make_async_remote_copy(
                src_ref=ag.at[par, 0], dst_ref=ag.at[par, ONE], send_sem=fw_send.at[par], recv_sem=fw_recv.at[par],
                device_id={'sx': row_id + ONE - TWO * parity}, device_id_type=MESH)

        def ag_third(par):
            waits(par, up_recv, n_chip - n_col)
            forward(par).start()

        def ag_done(par):
            waits(par, ag_send, n_col - ONE)
            waits(par, up_send, n_chip - n_col)
            forward(par).wait_send()

        def rows_sum(t):
            return jnp.sum(t, axis=0, keepdims=True)

        def pack_sides():
            for q in range(size // TWO):
                for c0, c1 in halves:
                    a, b = TWO * q * size, (TWO * q + ONE) * size
                    m = low4[:, :c1 - c0]
                    pack[0, SUB * q:SUB * q + SUB, c0:c1] = jnp.where(m, v[a:a + SUB, c0:c1], roll4(v[b:b + SUB, c0:c1]))
                    a, b = b - SUB, b + size - SUB
                    pack[ONE, SUB * q:SUB * q + SUB, c0:c1] = jnp.where(m, roll4(v[a:a + SUB, c0:c1]), v[b:b + SUB, c0:c1])
            sides = (pack.at[0], pack.at[ONE])
            for k, (src, first) in enumerate(((v, 0), (v, own - strip), (sides[0], 0), (sides[ONE], 0), (sides[0], 0), (sides[ONE], 0),
                                              (sides[0], strip - corner), (sides[ONE], strip - corner))):
                pack_message(h_out, q_off[k], src, first, h_len[k])

        f_copy.wait()
        r_copy.wait()
        pack_sides()
        each(h_copy, 'start')

        bt = split3(basis_t_ref[...])
        for i, part in enumerate(bt):
            stage[SUB * i:SUB * i + SUB, 0:own] = part.astype(F32)
        b_t[...] = stage[0:SUB * len(bt), 0:own].astype(BF16)

        def split_own(i):
            rows = pl.ds(pl.multiple_of(i * size, size), size)
            parts = split3(v[rows, :])
            for j, part in enumerate(parts):
                rp[j, rows, :] = part
        repeat(size, split_own, FOUR)

        def restrict(par):
            d1 = dot(b_t[...], rp[0, 0:own, :])
            d2 = dot(b_t[0:16, :], rp[1, 0:own, :])
            d3 = dot(b_t[0:16, :], rp[2, 0:own, :])
            d = (d1[16:24] + d2[8:16] + d3[0:8]) + (d1[8:16] + d2[0:8]) + d1[0:8]
            ags[par, SUB:TWO * SUB, :] = d[:, 0:LANES]
            ags[par, TWO * SUB:SLOT, 0:tail] = d[:, LANES:n_rhs]

        restrict(0)
        ags[0, 0:ONE, :] = count_ref[0:ONE, :]
        ag_start(0)

        for k in range(4):
            @pl.when(exists[k])
            def _(k=k):
                edge_in[k].wait_recv()
                edge_copy[k].wait_send()

        ag_second(0)

        def turn(count, col):
            for c0, c1 in tiles:
                turned = stage[0:count, c0:c1].T
                for n in range(c0, c1, 8):
                    perm[n // edge, n % edge:n % edge + 8, pl.ds(col, count)] = turned[n - c0:n - c0 + 8]

        def turn_band(jj):
            band_copy(jj).wait()
            for i in range(over):
                stage[size * i:size * i + size, :] = nat[over * jj + i, lo:hi, :]
            block = (jj + size // over + 1) % (size // over + 2)
            turn(strip, pl.multiple_of(block * strip, strip))
        repeat(edge // over, turn_band)
        for side, b0 in ((0, 0), (1, hi)):
            for i in range(size):
                stage[over * i:over * i + over, :] = nat[lo + i, b0:b0 + over, :]
            turn(strip, own + 2 * strip + side * strip)
        for q, (a0, b0) in enumerate(((0, 0), (0, hi), (hi, 0), (hi, hi))):
            for i in range(over):
                stage[corner * q + over * i:corner * q + over * i + over, :] = nat[a0 + i, b0:b0 + over, :]
        turn(k_corner, k_main)

        ag_third(0)

        def put_parts(rows, x, xc):
            parts = split3(x)
            for j, part in enumerate(parts):
                lp[j, rows, :] = part
            c = [t.astype(F32) for t in split3(xc)]
            order = (c[0], c[0], c[0], c[1], c[1], c[2])
            lc[rows, :] = jnp.concatenate(order, axis=1).astype(BF16)

        def put_own(i):
            rows = pl.ds(pl.multiple_of(batch1 + i * size, size), size)
            put_parts(rows, perm[lo + i, lo:hi, 0:k_main], perm[lo + i, lo:hi, k_main:ext])
        repeat(size, put_own)

        def take(at, a0, na, b0, nb_):
            for i in range(na):
                stage[at + nb_ * i:at + nb_ * i + nb_, :] = perm[a0 + i, b0:b0 + nb_, :]
            return at + na * nb_

        def take_col(at, a0, na, b):
            for i in range(na):
                stage[at + i:at + i + 1, :] = perm[a0 + i, b:b + 1, :]
            return at + na

        def flush(count, first):
            step = 48

            def go(i):
                src = pl.ds(pl.multiple_of(i * step, step), step)
                dst = pl.ds(pl.multiple_of(first + i * step, step), step)
                put_parts(dst, stage[src, 0:k_main], stage[src, k_main:ext])
            repeat(count // step, go)

        at = 0
        for a_strip, a_own in ((0, lo), (hi, hi - 1)):
            at = take(at, a_strip, over, lo, size)
            at = take(at, a_own, 1, lo, size)
            at = take_col(at, a_strip, over, lo - 1)
            at = take_col(at, a_strip, over, hi)
        flush(at, 0)
        at = 0
        for b_strip, b_own in ((0, lo), (hi, hi - 1)):
            at = take(at, lo, size, b_strip, over)
            at = take_col(at, lo, size, b_own)
            at = take(at, lo - 1, 1, b_strip, over)
            at = take(at, hi, 1, b_strip, over)
        flush(at, 2 * msg)
        at = 0
        for a_strip, a_own in ((0, lo), (hi, hi - 1)):
            for b_strip, b_own in ((0, lo), (hi, hi - 1)):
                at = take(at, a_strip, over, b_strip, over)
                at = take(at, a_own, 1, b_strip, over)
                at = take_col(at, a_strip, over, b_own)
        flush(at, 4 * msg)

        k5 = 5 * kmax

        def put_basis(i, first, x):
            parts = [t.astype(F32) for t in split3(x)]
            perm[i, 0:size, 0:256] = jnp.zeros((size, 256), F32)
            for c, (j, _) in enumerate(COMBOS):
                perm[i, 0:size, k5 * c + first:k5 * c + first + kmax] = parts[j]
            bcat[pl.ds(pl.multiple_of(i * size, size), size), :] = perm[i, 0:size, 0:256].astype(BF16)

        def put_basis_line(i):
            put_basis(i, 0, cell_ref[pl.ds(pl.multiple_of(i * size, size), size), LANES:LANES + kmax])
        repeat(size, put_basis_line, TWO)
        for k in range(4):
            put_basis(size + k, kmax * (k + 1), edges[k, :, LANES:LANES + kmax])
        coef[...] = jnp.zeros_like(coef)

        width = LANES
        sub_k = lax.broadcasted_iota(jnp.int32, (8, width), 0)
        for i in range(size):
            perm[i, 0:size, 0:width] = cell_ref[size * i:size * i + size, 0:width]
            perm[i, size:ring, 0:width] = jnp.where(sub_k == 0, edges[3, i:i + 1, 0:width], edges[2, i:i + 1, 0:width])
        perm[size, 0:size, 0:width] = edges[1, :, 0:width]
        perm[size + 1, 0:size, 0:width] = edges[0, :, 0:width]
        wn, ws, ww, we, wd = range(5)

        def harmonic(a, b):
            return 2.0 * a * b / (a + b)

        def put_weights(i):
            rows = pl.ds(pl.multiple_of(i * size, size), size)
            mid = perm[i, 0:ring, 0:width]
            up = perm[(i + size + 1) % (size + 2), 0:size, 0:width]
            down = perm[i + 1, 0:size, 0:width]
            here = mid[0:size]
            a = harmonic(here, up)
            b = harmonic(here, down)
            c = harmonic(here, pltpu.roll(mid, 1, 0)[0:size])
            d = harmonic(here, pltpu.roll(mid, ring - 1, 0)[0:size])
            scal[wn, rows, :] = a
            scal[ws, rows, :] = b
            scal[ww, rows, :] = c
            scal[we, rows, :] = d
            scal[wd, rows, :] = a + b + c + d
        repeat(size, put_weights, FOUR)

        forward(0).wait_recv()
        n_slot = n_dev * SLOT
        dev_rows = ag[0].reshape(n_dev, SLOT, LANES)[:, 0:ONE, 0:SUB]
        count_row = jnp.broadcast_to(dev_rows, (n_dev, SLOT, SUB)).reshape(n_slot, SUB).T
        count_dev = jnp.broadcast_to(dev_rows, (n_dev, SUB, SUB)).reshape(n_dev * SUB, SUB).T

        def floor_div(a, b):
            return jnp.floor((a + 0.5) * (ONE / b))

        def slot_facts(shape, axis, step=ONE):
            at = lax.broadcasted_iota(jnp.int32, shape, axis).astype(F32) * float(step)
            slot = floor_div(at, SLOT)
            inside = at - slot * SLOT
            other = floor_div(slot, n_chip)
            chip = slot - other * n_chip
            line = floor_div(chip, n_col)
            mine = parity.astype(F32)
            odd = mine + other - TWO * mine * other
            return (TWO * line + odd) * n_col + (chip - line * n_col), inside
        sub_r, inside_r = slot_facts((n_dev * SUB, n_slot), 0, SLOT // SUB)
        sub_c, _ = slot_facts((n_dev * SUB, n_slot), ONE)
        before = jnp.where(jnp.logical_and(inside_r == 0.0, sub_r < sub_c), 1.0, 0.0).astype(F32)
        start_row = dot_highest(count_dev, before)
        _, place = slot_facts((SUB, n_slot), ONE)
        which = lax.broadcasted_iota(jnp.int32, (ktot, n_slot), 0).astype(F32)

        def one_hot(first):
            here = place - first
            target = jnp.where(jnp.logical_and(here >= 0.0, here < count_row), start_row + here, -1.0)
            return jnp.where(which == target[0:ONE, :], 1.0, 0.0).astype(F32)
        pack_low, pack_high = one_hot(SUB), one_hot(TWO * SUB)
        k_row = lax.broadcasted_iota(jnp.int32, (k5, n_slot), 0).astype(F32)
        block = floor_div(k_row, kmax)
        sub_k, inside_k = slot_facts((k5, n_slot), ONE)
        wanted = me.astype(F32) + jnp.zeros((k5, n_slot), F32)
        present = block == 0.0
        for k in range(4):
            shift = DIRS[k][1] * n_col + DIRS[k][2]
            wanted = wanted + jnp.where(block == k + ONE, float(shift), 0.0)
            present = jnp.logical_or(present, jnp.logical_and(block == k + ONE, exists[k]))
        chosen = jnp.logical_and(sub_k == wanted, inside_k == SUB + k_row - block * kmax)
        select = jnp.where(jnp.logical_and(chosen, present), 1.0, 0.0).astype(F32)
        pick = lax.dot_general(select, pack_low, (((1,), (1,)), ((), ())), precision=lax.Precision.HIGHEST, preferred_element_type=F32)
        pick = dot_highest(pick, cinv_ref[...])
        c_map[0:k5, :] = dot_highest(pick, pack_low)
        c_map[k5:TWO * k5, :] = dot_highest(pick, pack_high)

        def field(par):
            for h, (c0, c1) in enumerate(halves):
                w_ = c1 - c0

                def line(i, sums):
                    rows = pl.ds(pl.multiple_of(i * size, size), size)
                    mid = z[i, :, c0:c1]
                    here = mid[0:size]
                    up = z[(i + size + ONE) % (size + TWO), 0:size, c0:c1]
                    down = z[i + ONE, 0:size, c0:c1]
                    left = pltpu.roll(mid, ONE, 0)[0:size]
                    right = pltpu.roll(mid, ring - ONE, 0)[0:size]
                    out = (scal[wd, rows, 0:w_] * here - scal[wn, rows, 0:w_] * up - scal[ws, rows, 0:w_] * down
                           - scal[ww, rows, 0:w_] * left - scal[we, rows, 0:w_] * right)
                    v[rows, c0:c1] = out
                    parts = split3(out)
                    for j, part in enumerate(parts):
                        rp[j, rows, c0:c1] = part
                    res = r[rows, c0:c1]
                    new = []
                    for total, t in zip(sums, (res * here, here * out, here * s[rows, c0:c1], res * res)):
                        q = t[0:SUB]
                        for n in range(SUB, size, SUB):
                            q = q + t[n:n + SUB]
                        new.append(total + q)
                    return tuple(new)

                def lines(i, sums):
                    for n in range(FOUR):
                        sums = line(i * FOUR + n, sums)
                    return sums
                sums = lax.fori_loop(0, size // FOUR, lines, tuple(jnp.zeros((SUB, w_), F32) for _ in range(FOUR)))
                for n in range(FOUR):
                    ags[par, FOUR * h + n:FOUR * h + n + ONE, 0:w_] = rows_sum(sums[n])

        def totals(par):
            return jnp.sum(ag[par].reshape(n_dev, SLOT, LANES)[:, 0:SUB, :], axis=0)

        def products(rows, k0, k1):
            out = None
            for i, j in COMBOS:
                t = dot(lp[i, rows, k0:k1], rp[j, k0:k1, :])
                out = t if out is None else out + t
            return out

        def scalars(par, it):
            t = totals(par)
            for h, (c0, c1) in enumerate(halves):
                rz, zw, zs, rr = [t[FOUR * h + n:FOUR * h + n + ONE, 0:c1 - c0] for n in range(FOUR)]
                nb[it, :, c0:c1] = jnp.broadcast_to(rr, (SUB, c1 - c0))
                old_rz, old_pq = cg[0, 0:ONE, c0:c1], cg[ONE, 0:ONE, c0:c1]
                first = it <= ONE
                beta = jnp.where(first, 0.0, rz / old_rz)
                pq = zw + jnp.where(first, 0.0, 2.0 * beta * zs + beta * beta * old_pq)
                for n, value in enumerate((rz, pq, rz / pq, beta)):
                    cg[n, 0:ONE, c0:c1] = value

        def advance():
            for c0, c1 in halves:
                alpha = cg[TWO, 0:ONE, c0:c1]
                beta = cg[3, 0:ONE, c0:c1]

                def line(i):
                    rows = pl.ds(pl.multiple_of(i * size, size), size)
                    new_p = z[i, 0:size, c0:c1] + beta * p[rows, c0:c1]
                    new_s = v[rows, c0:c1] + beta * s[rows, c0:c1]
                    p[rows, c0:c1] = new_p
                    s[rows, c0:c1] = new_s
                    x_ref[rows, c0:c1] = x_ref[rows, c0:c1] + alpha * new_p
                    r[rows, c0:c1] = r[rows, c0:c1] - alpha * new_s
                repeat(size, line, TWO)

        gn, gs, gw, ge, gnw, gne, gsw, gse = u_off

        def fold():
            mine = batch1
            for k in range(8):
                first, rows, at = u_off[k], u_len[k], m_off[k]
                left, _ = packed(rows)
                g[first:first + rows, 0:LANES] = g_raw[at:at + rows, :]
                at = at + rows
                g[first:first + left, LANES:n_rhs] = g_raw[at:at + left, 0:tail]
                g[first + left:first + rows, LANES:n_rhs] = g_raw[at:at + rows - left, LANES - tail:LANES]
            u[mine:mine + strip, :] = u[mine:mine + strip, :] + g[gn:gn + strip, :]
            u[mine + own - strip:mine + own, :] = u[mine + own - strip:mine + own, :] + g[gs:gs + strip, :]
            for side, first, last in ((gw, gnw, gsw), (ge, gne, gse)):
                g[side:side + corner, :] = g[side:side + corner, :] + g[first:first + corner, :]
                end = side + strip
                g[end - corner:end, :] = g[end - corner:end, :] + g[last:last + corner, :]

            def last_rows(k):
                first = u_off[k] + u_len[k] - 8
                return g[first:first + 8, :]
            t = [last_rows(k) for k in range(8)]
            n_, s_, w_, e_, nw, ne, sw, se = t

            def lower(a):
                return jnp.where(low4, a, 0.0)

            def upper(a):
                return jnp.where(low4, 0.0, a)

            edge_sum = [
                (g[gn + strip:gn + strip + size, :] + u[gn + strip - size:gn + strip, :], lower(w_ + nw), upper(roll4(e_) + roll4(ne))),
                (g[gs + strip:gs + strip + size, :] + u[gs:gs + size, :], lower(roll4(w_) + sw), upper(e_ + roll4(se))),
                (g[gw + strip:gw + strip + size, :], lower(n_ + roll4(nw)), upper(roll4(s_) + sw)),
                (g[ge + strip:ge + strip + size, :], lower(roll4(n_) + roll4(ne)), upper(s_ + se)),
            ]
            for k in range(4):
                base, first, last = edge_sum[k]
                ring_v[k] = base + mc[own + size * k:own + size * k + size, :]
                ring_v[k, 0:8, :] = ring_v[k, 0:8, :] + first
                ring_v[k, size - 8:size, :] = ring_v[k, size - 8:size, :] + last

            for c0, c1 in halves:
                w = c1 - c0
                alpha = cg[TWO, 0:ONE, c0:c1]
                beta = cg[3, 0:ONE, c0:c1]
                sub = sub8[:, :w]
                low = low4[:, :w]
                at_w = jnp.logical_and(sub == 7, exists[2])
                at_e = jnp.logical_and(sub == 0, exists[3])

                def push(i, a, b, m):
                    new = m + beta * ms[i, a:b, c0:c1]
                    ms[i, a:b, c0:c1] = new
                    z[i, a:b, c0:c1] = z[i, a:b, c0:c1] - alpha * new

                def eight_lines(b):
                    tile = pl.ds(pl.multiple_of(8 * b, 8), 8)
                    ring_w = ring_v[2, tile, c0:c1]
                    ring_e = ring_v[3, tile, c0:c1]
                    for line in range(8):
                        i = 8 * b + line
                        odd = line % 2
                        four = 4 * (i - odd)
                        if not odd:
                            tw = g[pl.ds(pl.multiple_of(gw + four, 8), 8), c0:c1]
                            te = g[pl.ds(pl.multiple_of(ge + four, 8), 8), c0:c1]
                            uw = u[pl.ds(pl.multiple_of(gw + four, 8), 8), c0:c1]
                            ue = u[pl.ds(pl.multiple_of(ge + four, 8), 8), c0:c1]
                        base = pl.multiple_of(i * size, size)
                        add_w = jnp.where(low, roll4(tw) if odd else tw, 0.0)
                        add_e = jnp.where(low, 0.0, te if odd else roll4(te))
                        for n in range(0, size, 8):
                            m = u[pl.ds(mine + base + n, 8), c0:c1] + mc[pl.ds(base + n, 8), c0:c1]
                            if n == 0:
                                m = m + add_w
                            if n == size - 8:
                                m = m + add_e
                            push(i, n, n + 8, m)
                        own_w = (uw if odd else roll4(uw)) + ring_w[line:line + 1]
                        own_e = (roll4(ue) if odd else ue) + ring_e[line:line + 1]
                        push(i, size, ring, jnp.where(at_w, own_w, jnp.where(at_e, own_e, 0.0)))
                repeat(size // SUB, eight_lines)
                push(size, 0, size, jnp.where(exists[1], ring_v[1, :, c0:c1], 0.0))
                push(size + 1, 0, size, jnp.where(exists[0], ring_v[0, :, c0:c1], 0.0))

        cg[...] = jnp.zeros_like(cg)
        first_rows = pl.ds(0, batch1)
        part_a = pl.ds(batch1, half_own)
        part_b = pl.ds(batch1 + half_own, half_own)

        def iteration(it):
            par = it % 2

            @pl.when(it > 0)
            def _():
                field(par)
                restrict(par)
                pack_sides()
                ag_start(par)
                each(h_copy, 'start')

            u[first_rows, :] = products(first_rows, 0, own)

            @pl.when(it > 0)
            def _():
                ag_second(par)
            u[part_a, :] = products(part_a, 0, own)
            each(h_in, 'recv')
            for k in range(8):
                rows, at = h_len[k], q_off[k]
                left, _ = packed(rows)
                upper = halo[at + rows:at + rows + left, :]
                low_parts = split3(halo[at:at + rows, :])
                high_parts = split3(jnp.concatenate([upper[:, 0:tail], upper[:, tail:LANES]], axis=0))
                if k < FOUR:
                    for j in range(3):
                        rp[j, own + h_off[k]:own + h_off[k] + rows, 0:LANES] = low_parts[j]
                        rp[j, own + h_off[k]:own + h_off[k] + rows, LANES:n_rhs] = high_parts[j]
                else:
                    for n, (_, j) in enumerate(COMBOS_C):
                        first = k_corner * n + h_off[k] - FOUR * strip
                        rc[first:first + rows, 0:LANES] = low_parts[j]
                        rc[first:first + rows, LANES:n_rhs] = high_parts[j]
            u[first_rows, :] = u[first_rows, :] + (products(first_rows, own, k_main) + dot(lc[first_rows, :], rc[...]))
            for k in range(8):
                pack_message(g_out, m_off[k], u, u_off[k], u_len[k])
            each(g_copy, 'start')
            u[part_a, :] = u[part_a, :] + (products(part_a, own, k_main) + dot(lc[part_a, :], rc[...]))

            @pl.when(it > 0)
            def _():
                ag_third(par)
            u[part_b, :] = products(part_b, 0, k_main) + dot(lc[part_b, :], rc[...])

            @pl.when(it > 0)
            def _():
                forward(par).wait_recv()
                scalars(par, it)
                advance()

            @pl.when(it == 0)
            def _():
                cg[TWO, 0:ONE, :] = jnp.full((ONE, n_rhs), -1.0, F32)

            c = dot_highest(c_map[...], ag[par].reshape(n_slot, LANES))
            for (c0, c1), value in zip(halves, (c[0:k5], c[k5:TWO * k5, 0:tail])):
                parts = split3(value)
                for n, (_, j) in enumerate(COMBOS):
                    coef[k5 * n:k5 * n + k5, c0:c1] = parts[j].astype(F32)
            mc[...] = dot(bcat[...], coef[...].astype(BF16))
            each(g_in, 'recv')
            fold()
            each(h_copy, 'sent')
            each(g_copy, 'sent')
            ag_done(par)
        repeat(ITERS, iteration)

        this, last = ITERS % TWO, (ITERS + ONE) % TWO
        field(this)
        ag_start(this)
        ag_second(this)
        ag_third(this)
        forward(this).wait_recv()
        scalars(this, ITERS)
        advance()
        for h, (c0, c1) in enumerate(halves):
            def line(i, total):
                res = r[pl.ds(pl.multiple_of(i * size, size), size), c0:c1]
                t = res * res
                for n in range(0, size, SUB):
                    total = total + t[n:n + SUB]
                return total
            total = lax.fori_loop(0, size, line, jnp.zeros((SUB, c1 - c0), F32))
            ags[last, FOUR * h + 3:FOUR * h + FOUR, 0:c1 - c0] = rows_sum(total)
        ag_start(last)
        ag_second(last)
        ag_third(last)
        forward(last).wait_recv()
        t = totals(last)
        for h, (c0, c1) in enumerate(halves):
            nb[ITERS + ONE, :, c0:c1] = jnp.broadcast_to(t[FOUR * h + 3:FOUR * h + FOUR, 0:c1 - c0], (SUB, c1 - c0))
        base_norm = jnp.sqrt(nb[ONE])
        for k in range(ITERS):
            norm_ref[k:k + ONE, :] = (jnp.sqrt(nb[k + TWO]) / base_norm)[0:ONE]
        ag_done(this)
        ag_done(last)

    COMBOS_C = ((0, 0), (0, 1), (0, 2), (1, 0), (1, 1), (2, 0))
    scratch = [
        pltpu.VMEM((edge, edge, ext), F32),
        pltpu.VMEM((edge, edge, ext), F32),
        pltpu.VMEM((2 * msg, ext), F32),
        pltpu.VMEM((3, rows_all, k_main), BF16),
        pltpu.VMEM((rows_all, 6 * k_corner), BF16),
        pltpu.VMEM((3, k_main, n_rhs), BF16),
        pltpu.VMEM((6 * k_corner, n_rhs), BF16),
        pltpu.VMEM((own, n_rhs), F32),
        pltpu.VMEM((2, strip, n_rhs), F32),
        pltpu.VMEM((sum(q_len), LANES), F32),
        pltpu.VMEM((sum(q_len), LANES), F32),
        pltpu.VMEM((rows_all, n_rhs), F32),
        pltpu.VMEM((sum(m_len), LANES), F32),
        pltpu.VMEM((sum(m_len), LANES), F32),
        pltpu.VMEM((batch1, n_rhs), F32),
        pltpu.VMEM((own, n_rhs), F32),
        pltpu.VMEM((own, n_rhs), F32),
        pltpu.VMEM((own, n_rhs), F32),
        pltpu.VMEM((size + 2, ring, n_rhs), F32),
        pltpu.VMEM((size + 2, ring, n_rhs), F32),
        pltpu.VMEM((own + 4 * size, n_rhs), F32),
        pltpu.VMEM((TWO, TWO, n_chip * SLOT, LANES), F32),
        pltpu.VMEM((TWO, SLOT, LANES), F32),
        pltpu.VMEM((own, TWO * LANES), F32),
        pltpu.VMEM((256, n_rhs), F32),
        pltpu.VMEM((own + 4 * size, 256), BF16),
        pltpu.VMEM((3 * kmax, own), BF16),
        pltpu.VMEM((10 * kmax, n_dev * SLOT), F32),
        pltpu.VMEM((4, size, 256), F32),
        pltpu.VMEM((2, size, 256), F32),
        pltpu.VMEM((4, size, n_rhs), F32),
        pltpu.VMEM((4, SUB, n_rhs), F32),
        pltpu.VMEM((ITERS + 2, 8, n_rhs), F32),
        pltpu.VMEM((5, own, 128), F32),
        pltpu.SemaphoreType.DMA((edge // over,)),
        pltpu.SemaphoreType.DMA((2,)),
        pltpu.SemaphoreType.DMA((4,)), pltpu.SemaphoreType.DMA((4,)),
        pltpu.SemaphoreType.DMA((8,)), pltpu.SemaphoreType.DMA((8,)),
        pltpu.SemaphoreType.DMA((8,)), pltpu.SemaphoreType.DMA((8,)),
    ] + [pltpu.SemaphoreType.DMA((TWO,))] * 6

    return kernel, scratch


def solution(mesh):
    n_row = mesh.shape['sx']
    n_col = mesh.shape['sy']

    def body(forcing, kappa, local_inv, coarse_basis, coarse_counts, coarse_inv):
        size = forcing.shape[0]
        n_rhs = forcing.shape[2]
        edge = math.isqrt(local_inv.shape[1])
        over = (edge - size) // 2
        kmax = coarse_basis.shape[2]
        ktot = coarse_inv.shape[0]
        own = size * size
        count = jnp.broadcast_to(coarse_counts.astype(F32)[:, None], (SUB, LANES))
        kernel, scratch = make_kernel(n_row, n_col, size, over, n_rhs, kmax, ktot)
        vmem = pl.BlockSpec(memory_space=pltpu.VMEM)
        hbm = pl.BlockSpec(memory_space=pl.ANY)
        solved, norms = pl.pallas_call(
            kernel,
            out_shape=(jax.ShapeDtypeStruct((own, n_rhs), F32), jax.ShapeDtypeStruct((ITERS, n_rhs), F32)),
            in_specs=[hbm, vmem, hbm, vmem, vmem, vmem],
            out_specs=(vmem, vmem),
            scratch_shapes=scratch,
            compiler_params=pltpu.CompilerParams(collective_id=0, has_side_effects=True, vmem_limit_bytes=67043328),
        )(forcing.reshape(own, n_rhs), kappa, local_inv.reshape(edge, edge, edge * edge), coarse_basis[0].T, count, coarse_inv)
        return solved.reshape(size, size, n_rhs), norms

    cell_spec = P(('batch', 'sx'), 'sy', None)
    sub_spec = P(('batch', 'sx', 'sy'), None, None)
    return jax.shard_map(body, mesh=mesh, in_specs=(cell_spec, P(('batch', 'sx'), 'sy'), sub_spec, sub_spec, P(('batch', 'sx', 'sy')), P('batch', None)), out_specs=(cell_spec, P('batch', None)), check_vma=False)
```

```python
import math
import jax
import jax.numpy as jnp
from jax import lax
from jax.experimental import pallas as pl
from jax.experimental.pallas import tpu as pltpu
from jax.sharding import PartitionSpec as P

ITERS = 8
MESH = pl.DeviceIdType.MESH
F32 = jnp.float32
BF16 = jnp.bfloat16
DIRS = (('N', -1, 0), ('S', 1, 0), ('W', 0, -1), ('E', 0, 1), ('NW', -1, -1), ('NE', -1, 1), ('SW', 1, -1), ('SE', 1, 1))
OPP = (1, 0, 3, 2, 7, 6, 5, 4)
COMBOS = ((0, 0), (0, 1), (1, 0), (0, 2), (1, 1), (2, 0))
ONE, TWO, FOUR, SUB, LANES = 1, 2, 4, 8, 128
SLOT = TWO * SUB
RZ, ZW, RR = SUB, SUB + ONE, SUB + TWO
TAIL_SUMS, TAIL_LAST = RR + ONE, RR + TWO
PAIRS = ((SUB - ONE, 0, ONE), (TAIL_LAST, None, TWO), (TAIL_LAST + ONE, 3, FOUR), (TAIL_LAST + TWO, 5, 6))


def repeat(count, body, by=ONE):
    def several(i, _):
        for n in range(by):
            body(i * by + n)
        return 0
    lax.fori_loop(0, count // by, several, 0)


def split3(x):
    high = x.astype(BF16)
    rest = x - high.astype(F32)
    mid = rest.astype(BF16)
    low = (rest - mid.astype(F32)).astype(BF16)
    return high, mid, low


def dot(a, b):
    return jnp.dot(a, b, preferred_element_type=F32)


def dot_highest(a, b):
    return jnp.dot(a, b, precision=lax.Precision.HIGHEST, preferred_element_type=F32)


def make_kernel(n_row, n_col, size, over, n_rhs, kmax, ktot):
    edge = size + 2 * over
    own = size * size
    strip = over * size
    corner = over * over
    ext = edge * edge
    n_dev = n_row * n_col
    lo, hi = over, over + size
    msg = strip + size + 2 * over
    cmsg = corner + 2 * over
    batch1 = 4 * msg + 4 * cmsg
    rows_all = batch1 + own
    k_main = own + 4 * strip
    k_corner = 4 * corner
    ring = size + 8
    u_off = [0, msg, 2 * msg, 3 * msg] + [4 * msg + cmsg * i for i in range(4)]
    u_len = [msg] * 4 + [cmsg] * 4
    h_off = [strip, 0, 2 * strip, 3 * strip] + [4 * strip + corner * i for i in range(4)]
    h_len = [strip] * 4 + [corner] * 4
    halves = ((0, LANES), (LANES, n_rhs))
    tail = n_rhs - LANES

    def packed(rows):
        left = -(-rows // (TWO * SUB)) * SUB
        return left, rows + left
    m_len = [packed(n)[ONE] for n in u_len]
    m_off = [sum(m_len[:k]) for k in range(8)]
    q_len = [packed(n)[ONE] for n in h_len]
    q_rank = (1, 0, 2, 3, 4, 5, 6, 7)
    q_off = [sum(q_len[j] for j in range(8) if q_rank[j] < q_rank[k]) for k in range(8)]
    tiles = [(c, min(c + 128, ext)) for c in range(0, ext, 128)]
    half_own = own // 2

    def kernel(f_hbm, kappa_ref, l_hbm, basis_t_ref, count_ref, cinv_ref,
               x_ref, norm_ref,
               nat, perm, stage, lp, lc, rp, rc, v, pack, h_out, halo, u, g_out, g_raw, g, r, p, s, ms, z, mc, ag, ags, cell_ref,
               coef, bcat, b_t, c_map, edges, pack_c, ring_v, cg, nb, scal,
               l_sem, f_sem, e_send, e_recv, h_send, h_recv, g_send, g_recv, ag_send, ag_recv):
        row_id = lax.axis_index('sx')
        col_id = lax.axis_index('sy')
        me = row_id * n_col + col_id

        def has(k):
            _, dr, dc = DIRS[k]
            ok = True
            for pos, step, count in ((row_id, dr, n_row), (col_id, dc, n_col)):
                if step < 0:
                    test = pos > 0
                elif step > 0:
                    test = pos < count - 1
                else:
                    continue
                ok = test if ok is True else jnp.logical_and(ok, test)
            return ok

        def there(k):
            return {'sx': row_id + DIRS[k][1], 'sy': col_id + DIRS[k][2]}

        exists = [has(k) for k in range(8)]

        def remote(src, dst, send, recv, k):
            return pltpu.make_async_remote_copy(src_ref=src, dst_ref=dst, send_sem=send, recv_sem=recv, device_id=there(k), device_id_type=MESH)

        def band_copy(j):
            lines = pl.ds(over * j, over)
            return pltpu.make_async_copy(l_hbm.at[lines], nat.at[lines], l_sem.at[j])
        for j in range(edge // over):
            band_copy(j).start()
        f_copy = pltpu.make_async_copy(f_hbm, v, f_sem.at[0])
        f_copy.start()
        r_copy = pltpu.make_async_copy(f_hbm, r, f_sem.at[1])
        r_copy.start()

        for ref in (halo, g_raw, g_out, ags, p, s, ms, z, x_ref):
            ref[...] = jnp.zeros_like(ref)
        eye = lax.broadcasted_iota(jnp.int32, (size, size), 0) == lax.broadcasted_iota(jnp.int32, (size, size), ONE)
        for i in range(size):
            diagonal = jnp.where(eye, kappa_ref[i:i + ONE, :], 0.0)
            cell_ref[size * i:size * i + size, 0:LANES] = jnp.broadcast_to(jnp.sum(diagonal, axis=ONE, keepdims=True), (size, LANES))
        for c in range(0, own, LANES):
            cell_ref[c:c + LANES, LANES:LANES + kmax] = basis_t_ref[:, c:c + LANES].T
        for i in range(size):
            pack_c[0, i:i + 1, :] = cell_ref[size * i:size * i + 1, :]
            pack_c[1, i:i + 1, :] = cell_ref[size * i + size - 1:size * i + size, :]
        edges[0] = cell_ref[0:size, :]
        edges[1] = cell_ref[own - size:own, :]
        edges[2] = pack_c[0]
        edges[3] = pack_c[1]

        barrier = pltpu.get_barrier_semaphore()

        for d in range(ONE, n_dev):
            peer = (me + d) % n_dev
            pl.semaphore_signal(barrier, inc=ONE, device_id={'sx': peer // n_col, 'sy': peer % n_col}, device_id_type=MESH)
        pl.semaphore_wait(barrier, n_dev - 1)

        edge_src = [cell_ref.at[pl.ds(0, size)], cell_ref.at[pl.ds(own - size, size)], pack_c.at[0], pack_c.at[1]]
        edge_copy = [remote(edge_src[k], edges.at[OPP[k]], e_send.at[k], e_recv.at[OPP[k]], k) for k in range(4)]
        edge_in = [remote(edge_src[k], edges.at[k], e_send.at[k], e_recv.at[k], k) for k in range(4)]
        for k in range(4):
            @pl.when(exists[k])
            def _(k=k):
                edge_copy[k].start()

        sub8 = lax.broadcasted_iota(jnp.int32, (8, n_rhs), 0)
        low4 = sub8 < 4

        def roll4(t):
            return pltpu.roll(t, 4, 0)

        def slices(ref, off, length):
            return [ref.at[pl.ds(off[k], length[k])] for k in range(8)]
        h_src, h_dst = slices(h_out, q_off, q_len), slices(halo, q_off, q_len)
        h_copy = [remote(h_src[k], h_dst[OPP[k]], h_send.at[k], h_recv.at[OPP[k]], k) for k in range(8)]
        h_in = [remote(h_src[k], h_dst[k], h_send.at[k], h_recv.at[k], k) for k in range(8)]
        g_src, g_dst = slices(g_out, m_off, m_len), slices(g_raw, m_off, m_len)
        g_copy = [remote(g_src[k], g_dst[OPP[k]], g_send.at[k], g_recv.at[OPP[k]], k) for k in range(8)]
        g_in = [remote(g_src[k], g_dst[k], g_send.at[k], g_recv.at[k], k) for k in range(8)]

        def pack_message(out, at, src, first, rows):
            left, _ = packed(rows)
            out[at:at + rows, :] = src[first:first + rows, 0:LANES]
            at = at + rows
            out[at:at + left, 0:tail] = src[first:first + left, LANES:n_rhs]
            out[at:at + rows - left, LANES - tail:LANES] = src[first + left:first + rows, LANES:n_rhs]

        def each(copies, what):
            for k in (2, 3, 0, 1, 4, 5, 6, 7):
                @pl.when(exists[k])
                def _(k=k):
                    if what == 'start':
                        copies[k].start()
                    elif what == 'recv':
                        copies[k].wait_recv()
                    else:
                        copies[k].wait_send()

        def ag_start(par, first=0):
            rows = SLOT - first
            mine = pl.ds(pl.multiple_of(me * SLOT + first, SUB), rows)
            ag[par, mine, :] = ags[par, first:SLOT, :]
            for d in range(ONE, n_dev):
                peer = (me + d) % n_dev
                pltpu.make_async_remote_copy(
                    src_ref=ags.at[par, pl.ds(first, rows)], dst_ref=ag.at[par, mine], send_sem=ag_send.at[par], recv_sem=ag_recv.at[par],
                    device_id={'sx': peer // n_col, 'sy': peer % n_col}, device_id_type=MESH).start()

        def ag_wait(par, sem, rows=SLOT):
            many = ag.at[par, pl.ds(0, (n_dev - ONE) * rows)]
            pltpu.make_async_copy(many, many, sem.at[par]).wait()

        def rows_sum(t):
            return jnp.sum(t, axis=0, keepdims=True)

        def pack_sides():
            for q in range(size // TWO):
                for c0, c1 in halves:
                    a, b = TWO * q * size, (TWO * q + ONE) * size
                    m = low4[:, :c1 - c0]
                    pack[0, SUB * q:SUB * q + SUB, c0:c1] = jnp.where(m, v[a:a + SUB, c0:c1], roll4(v[b:b + SUB, c0:c1]))
                    a, b = b - SUB, b + size - SUB
                    pack[ONE, SUB * q:SUB * q + SUB, c0:c1] = jnp.where(m, roll4(v[a:a + SUB, c0:c1]), v[b:b + SUB, c0:c1])
            sides = (pack.at[0], pack.at[ONE])
            for k, (src, first) in enumerate(((v, 0), (v, own - strip), (sides[0], 0), (sides[ONE], 0), (sides[0], 0), (sides[ONE], 0),
                                              (sides[0], strip - corner), (sides[ONE], strip - corner))):
                pack_message(h_out, q_off[k], src, first, h_len[k])

        f_copy.wait()
        r_copy.wait()
        pack_sides()
        each(h_copy, 'start')

        bt = split3(basis_t_ref[...])
        for i, part in enumerate(bt):
            stage[SUB * i:SUB * i + SUB, 0:own] = part.astype(F32)
        b_t[...] = stage[0:SUB * len(bt), 0:own].astype(BF16)

        def split_own(i):
            rows = pl.ds(pl.multiple_of(i * size, size), size)
            parts = split3(v[rows, :])
            for j, part in enumerate(parts):
                rp[j, rows, :] = part
        repeat(size, split_own, FOUR)

        def restrict(par):
            d1 = dot(b_t[...], rp[0, 0:own, :])
            d2 = dot(b_t[0:16, :], rp[1, 0:own, :])
            d3 = dot(b_t[0:16, :], rp[2, 0:own, :])
            d = (d1[16:24] + d2[8:16] + d3[0:8]) + (d1[8:16] + d2[0:8]) + d1[0:8]
            ags[par, 0:SUB - ONE, :] = d[0:SUB - ONE, 0:LANES]
            for row, left, right in PAIRS:
                if left is not None:
                    ags[par, row:row + ONE, 0:tail] = d[left:left + ONE, LANES:n_rhs]
                ags[par, row:row + ONE, tail:LANES] = d[right:right + ONE, LANES:n_rhs]

        restrict(0)
        ags[0, RZ:ZW, :] = count_ref[0:ONE, :]
        ag_start(0)

        for k in range(4):
            @pl.when(exists[k])
            def _(k=k):
                edge_in[k].wait_recv()
                edge_copy[k].wait_send()

        def turn(count, col):
            for c0, c1 in tiles:
                turned = stage[0:count, c0:c1].T
                for n in range(c0, c1, 8):
                    perm[n // edge, n % edge:n % edge + 8, pl.ds(col, count)] = turned[n - c0:n - c0 + 8]

        def turn_band(jj):
            band_copy(jj).wait()
            for i in range(over):
                stage[size * i:size * i + size, :] = nat[over * jj + i, lo:hi, :]
            block = (jj + size // over + 1) % (size // over + 2)
            turn(strip, pl.multiple_of(block * strip, strip))
        repeat(edge // over, turn_band)
        for side, b0 in ((0, 0), (1, hi)):
            for i in range(size):
                stage[over * i:over * i + over, :] = nat[lo + i, b0:b0 + over, :]
            turn(strip, own + 2 * strip + side * strip)
        for q, (a0, b0) in enumerate(((0, 0), (0, hi), (hi, 0), (hi, hi))):
            for i in range(over):
                stage[corner * q + over * i:corner * q + over * i + over, :] = nat[a0 + i, b0:b0 + over, :]
        turn(k_corner, k_main)

        def put_parts(rows, x, xc):
            parts = split3(x)
            for j, part in enumerate(parts):
                lp[j, rows, :] = part
            c = [t.astype(F32) for t in split3(xc)]
            order = (c[0], c[0], c[0], c[1], c[1], c[2])
            lc[rows, :] = jnp.concatenate(order, axis=1).astype(BF16)

        def put_own(i):
            rows = pl.ds(pl.multiple_of(batch1 + i * size, size), size)
            put_parts(rows, perm[lo + i, lo:hi, 0:k_main], perm[lo + i, lo:hi, k_main:ext])
        repeat(size, put_own)

        def take(at, a0, na, b0, nb_):
            for i in range(na):
                stage[at + nb_ * i:at + nb_ * i + nb_, :] = perm[a0 + i, b0:b0 + nb_, :]
            return at + na * nb_

        def take_col(at, a0, na, b):
            for i in range(na):
                stage[at + i:at + i + 1, :] = perm[a0 + i, b:b + 1, :]
            return at + na

        def flush(count, first):
            step = 48

            def go(i):
                src = pl.ds(pl.multiple_of(i * step, step), step)
                dst = pl.ds(pl.multiple_of(first + i * step, step), step)
                put_parts(dst, stage[src, 0:k_main], stage[src, k_main:ext])
            repeat(count // step, go)

        at = 0
        for a_strip, a_own in ((0, lo), (hi, hi - 1)):
            at = take(at, a_strip, over, lo, size)
            at = take(at, a_own, 1, lo, size)
            at = take_col(at, a_strip, over, lo - 1)
            at = take_col(at, a_strip, over, hi)
        flush(at, 0)
        at = 0
        for b_strip, b_own in ((0, lo), (hi, hi - 1)):
            at = take(at, lo, size, b_strip, over)
            at = take_col(at, lo, size, b_own)
            at = take(at, lo - 1, 1, b_strip, over)
            at = take(at, hi, 1, b_strip, over)
        flush(at, 2 * msg)
        at = 0
        for a_strip, a_own in ((0, lo), (hi, hi - 1)):
            for b_strip, b_own in ((0, lo), (hi, hi - 1)):
                at = take(at, a_strip, over, b_strip, over)
                at = take(at, a_own, 1, b_strip, over)
                at = take_col(at, a_strip, over, b_own)
        flush(at, 4 * msg)

        k5 = 5 * kmax

        def put_basis(i, first, x):
            parts = [t.astype(F32) for t in split3(x)]
            perm[i, 0:size, 0:256] = jnp.zeros((size, 256), F32)
            for c, (j, _) in enumerate(COMBOS):
                perm[i, 0:size, k5 * c + first:k5 * c + first + kmax] = parts[j]
            bcat[pl.ds(pl.multiple_of(i * size, size), size), :] = perm[i, 0:size, 0:256].astype(BF16)

        def put_basis_line(i):
            put_basis(i, 0, cell_ref[pl.ds(pl.multiple_of(i * size, size), size), LANES:LANES + kmax])
        repeat(size, put_basis_line, TWO)
        for k in range(4):
            put_basis(size + k, kmax * (k + 1), edges[k, :, LANES:LANES + kmax])
        coef[...] = jnp.zeros_like(coef)

        width = LANES
        sub_k = lax.broadcasted_iota(jnp.int32, (8, width), 0)
        for i in range(size):
            perm[i, 0:size, 0:width] = cell_ref[size * i:size * i + size, 0:width]
            perm[i, size:ring, 0:width] = jnp.where(sub_k == 0, edges[3, i:i + 1, 0:width], edges[2, i:i + 1, 0:width])
        perm[size, 0:size, 0:width] = edges[1, :, 0:width]
        perm[size + 1, 0:size, 0:width] = edges[0, :, 0:width]
        wn, ws, ww, we, wd = range(5)

        def harmonic(a, b):
            return 2.0 * a * b / (a + b)

        def put_weights(i):
            rows = pl.ds(pl.multiple_of(i * size, size), size)
            mid = perm[i, 0:ring, 0:width]
            up = perm[(i + size + 1) % (size + 2), 0:size, 0:width]
            down = perm[i + 1, 0:size, 0:width]
            here = mid[0:size]
            a = harmonic(here, up)
            b = harmonic(here, down)
            c = harmonic(here, pltpu.roll(mid, 1, 0)[0:size])
            d = harmonic(here, pltpu.roll(mid, ring - 1, 0)[0:size])
            scal[wn, rows, :] = a
            scal[ws, rows, :] = b
            scal[ww, rows, :] = c
            scal[we, rows, :] = d
            scal[wd, rows, :] = a + b + c + d
        repeat(size, put_weights, FOUR)

        ag_wait(0, ag_recv)
        n_slot = n_dev * SLOT
        dev_rows = ag[0].reshape(n_dev, SLOT, LANES)[:, RZ:ZW, 0:SUB]
        count_row = jnp.broadcast_to(dev_rows, (n_dev, SLOT, SUB)).reshape(n_slot, SUB).T
        count_dev = jnp.broadcast_to(dev_rows, (n_dev, SUB, SUB)).reshape(n_dev * SUB, SUB).T

        def floor_div(a, b):
            return jnp.floor((a + 0.5) * (ONE / b))

        def slot_facts(shape, axis, step=ONE):
            at = lax.broadcasted_iota(jnp.int32, shape, axis).astype(F32) * float(step)
            slot = floor_div(at, SLOT)
            inside = at - slot * SLOT
            return slot, inside
        sub_r, inside_r = slot_facts((n_dev * SUB, n_slot), 0, SLOT // SUB)
        sub_c, _ = slot_facts((n_dev * SUB, n_slot), ONE)
        before = jnp.where(jnp.logical_and(inside_r == 0.0, sub_r < sub_c), 1.0, 0.0).astype(F32)
        start_row = dot_highest(count_dev, before)
        _, place = slot_facts((SUB, n_slot), ONE)
        which = lax.broadcasted_iota(jnp.int32, (ktot, n_slot), 0).astype(F32)

        def one_hot(here):
            target = jnp.where(jnp.logical_and(here >= 0.0, here < count_row), start_row + here, -1.0)
            return jnp.where(which == target[0:ONE, :], 1.0, 0.0).astype(F32)
        pack_low = one_hot(place)
        at_left = at_right = jnp.full_like(place, -1.0)
        for row, left, right in PAIRS:
            if left is not None:
                at_left = jnp.where(place == float(row), float(left), at_left)
            at_right = jnp.where(place == float(row), float(right), at_right)
        k_row = lax.broadcasted_iota(jnp.int32, (k5, n_slot), 0).astype(F32)
        block = floor_div(k_row, kmax)
        sub_k, inside_k = slot_facts((k5, n_slot), ONE)
        wanted = me.astype(F32) + jnp.zeros((k5, n_slot), F32)
        present = block == 0.0
        for k in range(4):
            shift = DIRS[k][1] * n_col + DIRS[k][2]
            wanted = wanted + jnp.where(block == k + ONE, float(shift), 0.0)
            present = jnp.logical_or(present, jnp.logical_and(block == k + ONE, exists[k]))
        chosen = jnp.logical_and(sub_k == wanted, inside_k == k_row - block * kmax)
        select = jnp.where(jnp.logical_and(chosen, present), 1.0, 0.0).astype(F32)
        pick = lax.dot_general(select, pack_low, (((1,), (1,)), ((), ())), precision=lax.Precision.HIGHEST, preferred_element_type=F32)
        pick = dot_highest(pick, cinv_ref[...])
        for n, onto in enumerate((pack_low, one_hot(at_left), one_hot(at_right))):
            c_map[k5 * n:k5 * n + k5, :] = dot_highest(pick, onto)

        SUMS = (RZ, ZW, RR)

        def place_of(h, row):
            if not h:
                return slice(row, row + ONE), slice(0, LANES)
            at = TAIL_LAST if row == RR else TAIL_SUMS
            return slice(at, at + ONE), (slice(tail, LANES) if row == ZW else slice(0, tail))

        def put_sum(par, h, row, value):
            rows, lanes = place_of(h, row)
            ags[par, rows, lanes] = value

        def field(par):
            for h, (c0, c1) in enumerate(halves):
                w_ = c1 - c0

                def line(i, sums):
                    rows = pl.ds(pl.multiple_of(i * size, size), size)
                    mid = z[i, :, c0:c1]
                    here = mid[0:size]
                    up = z[(i + size + ONE) % (size + TWO), 0:size, c0:c1]
                    down = z[i + ONE, 0:size, c0:c1]
                    left = pltpu.roll(mid, ONE, 0)[0:size]
                    right = pltpu.roll(mid, ring - ONE, 0)[0:size]
                    out = (scal[wd, rows, 0:w_] * here - scal[wn, rows, 0:w_] * up - scal[ws, rows, 0:w_] * down
                           - scal[ww, rows, 0:w_] * left - scal[we, rows, 0:w_] * right)
                    v[rows, c0:c1] = out
                    parts = split3(out)
                    for j, part in enumerate(parts):
                        rp[j, rows, c0:c1] = part
                    res = r[rows, c0:c1]
                    new = []
                    for total, t in zip(sums, (res * here, here * out, res * res)):
                        q = t[0:SUB]
                        for n in range(SUB, size, SUB):
                            q = q + t[n:n + SUB]
                        new.append(total + q)
                    return tuple(new)

                def lines(i, sums):
                    for n in range(FOUR):
                        sums = line(i * FOUR + n, sums)
                    return sums
                sums = lax.fori_loop(0, size // FOUR, lines, tuple(jnp.zeros((SUB, w_), F32) for _ in SUMS))
                for n, total in zip(SUMS, sums):
                    put_sum(par, h, n, rows_sum(total))

        def totals(par):
            t = jnp.sum(ag[par].reshape(n_dev, SLOT, LANES)[:, SUB:SLOT, :], axis=0)

            def get(h, row):
                rows, lanes = place_of(h, row)
                return t[rows.start - SUB:rows.stop - SUB, lanes]
            return get

        def products(rows, k0, k1):
            out = None
            for i, j in COMBOS:
                t = dot(lp[i, rows, k0:k1], rp[j, k0:k1, :])
                out = t if out is None else out + t
            return out

        def scalars(par, it):
            t = totals(par)
            for h, (c0, c1) in enumerate(halves):
                rz, zw, rr = [t(h, row) for row in SUMS]
                nb[it, :, c0:c1] = jnp.broadcast_to(rr, (SUB, c1 - c0))
                old_rz, old_pq = cg[0, 0:ONE, c0:c1], cg[ONE, 0:ONE, c0:c1]
                first = it <= ONE
                beta = jnp.where(first, 0.0, rz / old_rz)
                pq = zw - jnp.where(first, 0.0, beta * beta * old_pq)
                for n, value in enumerate((rz, pq, rz / pq, beta)):
                    cg[n, 0:ONE, c0:c1] = value

        def advance():
            for c0, c1 in halves:
                alpha = cg[TWO, 0:ONE, c0:c1]
                beta = cg[3, 0:ONE, c0:c1]

                def line(i):
                    rows = pl.ds(pl.multiple_of(i * size, size), size)
                    new_p = z[i, 0:size, c0:c1] + beta * p[rows, c0:c1]
                    new_s = v[rows, c0:c1] + beta * s[rows, c0:c1]
                    p[rows, c0:c1] = new_p
                    s[rows, c0:c1] = new_s
                    x_ref[rows, c0:c1] = x_ref[rows, c0:c1] + alpha * new_p
                    r[rows, c0:c1] = r[rows, c0:c1] - alpha * new_s
                repeat(size, line, TWO)

        gn, gs, gw, ge, gnw, gne, gsw, gse = u_off

        def fold():
            mine = batch1
            for k in range(8):
                first, rows, at = u_off[k], u_len[k], m_off[k]
                left, _ = packed(rows)
                g[first:first + rows, 0:LANES] = g_raw[at:at + rows, :]
                at = at + rows
                g[first:first + left, LANES:n_rhs] = g_raw[at:at + left, 0:tail]
                g[first + left:first + rows, LANES:n_rhs] = g_raw[at:at + rows - left, LANES - tail:LANES]
            u[mine:mine + strip, :] = u[mine:mine + strip, :] + g[gn:gn + strip, :]
            u[mine + own - strip:mine + own, :] = u[mine + own - strip:mine + own, :] + g[gs:gs + strip, :]
            for side, first, last in ((gw, gnw, gsw), (ge, gne, gse)):
                g[side:side + corner, :] = g[side:side + corner, :] + g[first:first + corner, :]
                end = side + strip
                g[end - corner:end, :] = g[end - corner:end, :] + g[last:last + corner, :]

            def last_rows(k):
                first = u_off[k] + u_len[k] - 8
                return g[first:first + 8, :]
            t = [last_rows(k) for k in range(8)]
            n_, s_, w_, e_, nw, ne, sw, se = t

            def lower(a):
                return jnp.where(low4, a, 0.0)

            def upper(a):
                return jnp.where(low4, 0.0, a)

            edge_sum = [
                (g[gn + strip:gn + strip + size, :] + u[gn + strip - size:gn + strip, :], lower(w_ + nw), upper(roll4(e_) + roll4(ne))),
                (g[gs + strip:gs + strip + size, :] + u[gs:gs + size, :], lower(roll4(w_) + sw), upper(e_ + roll4(se))),
                (g[gw + strip:gw + strip + size, :], lower(n_ + roll4(nw)), upper(roll4(s_) + sw)),
                (g[ge + strip:ge + strip + size, :], lower(roll4(n_) + roll4(ne)), upper(s_ + se)),
            ]
            for k in range(4):
                base, first, last = edge_sum[k]
                ring_v[k] = base + mc[own + size * k:own + size * k + size, :]
                ring_v[k, 0:8, :] = ring_v[k, 0:8, :] + first
                ring_v[k, size - 8:size, :] = ring_v[k, size - 8:size, :] + last

            for c0, c1 in halves:
                w = c1 - c0
                alpha = cg[TWO, 0:ONE, c0:c1]
                beta = cg[3, 0:ONE, c0:c1]
                sub = sub8[:, :w]
                low = low4[:, :w]
                at_w = jnp.logical_and(sub == 7, exists[2])
                at_e = jnp.logical_and(sub == 0, exists[3])

                def push(i, a, b, m):
                    new = m + beta * ms[i, a:b, c0:c1]
                    ms[i, a:b, c0:c1] = new
                    z[i, a:b, c0:c1] = z[i, a:b, c0:c1] - alpha * new

                def eight_lines(b):
                    tile = pl.ds(pl.multiple_of(8 * b, 8), 8)
                    ring_w = ring_v[2, tile, c0:c1]
                    ring_e = ring_v[3, tile, c0:c1]
                    for line in range(8):
                        i = 8 * b + line
                        odd = line % 2
                        four = 4 * (i - odd)
                        if not odd:
                            tw = g[pl.ds(pl.multiple_of(gw + four, 8), 8), c0:c1]
                            te = g[pl.ds(pl.multiple_of(ge + four, 8), 8), c0:c1]
                            uw = u[pl.ds(pl.multiple_of(gw + four, 8), 8), c0:c1]
                            ue = u[pl.ds(pl.multiple_of(ge + four, 8), 8), c0:c1]
                        base = pl.multiple_of(i * size, size)
                        add_w = jnp.where(low, roll4(tw) if odd else tw, 0.0)
                        add_e = jnp.where(low, 0.0, te if odd else roll4(te))
                        for n in range(0, size, 8):
                            m = u[pl.ds(mine + base + n, 8), c0:c1] + mc[pl.ds(base + n, 8), c0:c1]
                            if n == 0:
                                m = m + add_w
                            if n == size - 8:
                                m = m + add_e
                            push(i, n, n + 8, m)
                        own_w = (uw if odd else roll4(uw)) + ring_w[line:line + 1]
                        own_e = (roll4(ue) if odd else ue) + ring_e[line:line + 1]
                        push(i, size, ring, jnp.where(at_w, own_w, jnp.where(at_e, own_e, 0.0)))
                repeat(size // SUB, eight_lines)
                push(size, 0, size, jnp.where(exists[1], ring_v[1, :, c0:c1], 0.0))
                push(size + 1, 0, size, jnp.where(exists[0], ring_v[0, :, c0:c1], 0.0))

        cg[...] = jnp.zeros_like(cg)
        first_rows = pl.ds(0, batch1)
        part_a = pl.ds(batch1, half_own)
        part_b = pl.ds(batch1 + half_own, half_own)

        def iteration(it):
            par = it % 2

            @pl.when(it > 0)
            def _():
                field(par)
                pack_sides()
                each(h_copy, 'start')
                restrict(par)
                ag_start(par)

            u[first_rows, :] = products(first_rows, 0, own)
            u[part_a, :] = products(part_a, 0, own)
            each(h_in, 'recv')
            for k in range(8):
                rows, at = h_len[k], q_off[k]
                left, _ = packed(rows)
                upper = halo[at + rows:at + rows + left, :]
                low_parts = split3(halo[at:at + rows, :])
                high_parts = split3(jnp.concatenate([upper[:, 0:tail], upper[:, tail:LANES]], axis=0))
                if k < FOUR:
                    for j in range(3):
                        rp[j, own + h_off[k]:own + h_off[k] + rows, 0:LANES] = low_parts[j]
                        rp[j, own + h_off[k]:own + h_off[k] + rows, LANES:n_rhs] = high_parts[j]
                else:
                    for n, (_, j) in enumerate(COMBOS_C):
                        first = k_corner * n + h_off[k] - FOUR * strip
                        rc[first:first + rows, 0:LANES] = low_parts[j]
                        rc[first:first + rows, LANES:n_rhs] = high_parts[j]
            u[first_rows, :] = u[first_rows, :] + (products(first_rows, own, k_main) + dot(lc[first_rows, :], rc[...]))
            for k in range(8):
                pack_message(g_out, m_off[k], u, u_off[k], u_len[k])
            each(g_copy, 'start')
            u[part_a, :] = u[part_a, :] + (products(part_a, own, k_main) + dot(lc[part_a, :], rc[...]))
            u[part_b, :] = products(part_b, 0, k_main) + dot(lc[part_b, :], rc[...])

            @pl.when(it > 0)
            def _():
                ag_wait(par, ag_recv)
                scalars(par, it)
                advance()

            @pl.when(it == 0)
            def _():
                cg[TWO, 0:ONE, :] = jnp.full((ONE, n_rhs), -1.0, F32)

            c = dot_highest(c_map[...], ag[par])
            for (c0, c1), value in zip(halves, (c[0:k5], c[k5:TWO * k5, 0:tail] + c[TWO * k5:, tail:LANES])):
                parts = split3(value)
                for n, (_, j) in enumerate(COMBOS):
                    coef[k5 * n:k5 * n + k5, c0:c1] = parts[j].astype(F32)
            mc[...] = dot(bcat[...], coef[...].astype(BF16))
            each(g_in, 'recv')
            fold()
            each(h_copy, 'sent')
            each(g_copy, 'sent')
            ag_wait(par, ag_send)
        repeat(ITERS, iteration)

        this, last = ITERS % TWO, (ITERS + ONE) % TWO
        field(this)
        ag_start(this, SUB)
        ag_wait(this, ag_recv, SUB)
        scalars(this, ITERS)
        advance()
        for h, (c0, c1) in enumerate(halves):
            def line(i, total):
                res = r[pl.ds(pl.multiple_of(i * size, size), size), c0:c1]
                t = res * res
                for n in range(0, size, SUB):
                    total = total + t[n:n + SUB]
                return total
            total = lax.fori_loop(0, size, line, jnp.zeros((SUB, c1 - c0), F32))
            put_sum(last, h, RR, rows_sum(total))
        ag_start(last, SUB)
        ag_wait(last, ag_recv, SUB)
        t = totals(last)
        for h, (c0, c1) in enumerate(halves):
            nb[ITERS + ONE, :, c0:c1] = jnp.broadcast_to(t(h, RR), (SUB, c1 - c0))
        base_norm = jnp.sqrt(nb[ONE])
        for k in range(ITERS):
            norm_ref[k:k + ONE, :] = (jnp.sqrt(nb[k + TWO]) / base_norm)[0:ONE]
        ag_wait(this, ag_send, SUB)
        ag_wait(last, ag_send, SUB)

    COMBOS_C = ((0, 0), (0, 1), (0, 2), (1, 0), (1, 1), (2, 0))
    scratch = [
        pltpu.VMEM((edge, edge, ext), F32),
        pltpu.VMEM((edge, edge, ext), F32),
        pltpu.VMEM((2 * msg, ext), F32),
        pltpu.VMEM((3, rows_all, k_main), BF16),
        pltpu.VMEM((rows_all, 6 * k_corner), BF16),
        pltpu.VMEM((3, k_main, n_rhs), BF16),
        pltpu.VMEM((6 * k_corner, n_rhs), BF16),
        pltpu.VMEM((own, n_rhs), F32),
        pltpu.VMEM((2, strip, n_rhs), F32),
        pltpu.VMEM((sum(q_len), LANES), F32),
        pltpu.VMEM((sum(q_len), LANES), F32),
        pltpu.VMEM((rows_all, n_rhs), F32),
        pltpu.VMEM((sum(m_len), LANES), F32),
        pltpu.VMEM((sum(m_len), LANES), F32),
        pltpu.VMEM((batch1, n_rhs), F32),
        pltpu.VMEM((own, n_rhs), F32),
        pltpu.VMEM((own, n_rhs), F32),
        pltpu.VMEM((own, n_rhs), F32),
        pltpu.VMEM((size + 2, ring, n_rhs), F32),
        pltpu.VMEM((size + 2, ring, n_rhs), F32),
        pltpu.VMEM((own + 4 * size, n_rhs), F32),
        pltpu.VMEM((TWO, n_dev * SLOT, LANES), F32),
        pltpu.VMEM((TWO, SLOT, LANES), F32),
        pltpu.VMEM((own, TWO * LANES), F32),
        pltpu.VMEM((256, n_rhs), F32),
        pltpu.VMEM((own + 4 * size, 256), BF16),
        pltpu.VMEM((3 * kmax, own), BF16),
        pltpu.VMEM((15 * kmax, n_dev * SLOT), F32),
        pltpu.VMEM((4, size, 256), F32),
        pltpu.VMEM((2, size, 256), F32),
        pltpu.VMEM((4, size, n_rhs), F32),
        pltpu.VMEM((4, SUB, n_rhs), F32),
        pltpu.VMEM((ITERS + 2, 8, n_rhs), F32),
        pltpu.VMEM((5, own, 128), F32),
        pltpu.SemaphoreType.DMA((edge // over,)),
        pltpu.SemaphoreType.DMA((2,)),
        pltpu.SemaphoreType.DMA((4,)), pltpu.SemaphoreType.DMA((4,)),
        pltpu.SemaphoreType.DMA((8,)), pltpu.SemaphoreType.DMA((8,)),
        pltpu.SemaphoreType.DMA((8,)), pltpu.SemaphoreType.DMA((8,)),
    ] + [pltpu.SemaphoreType.DMA((TWO,))] * 2

    return kernel, scratch


def solution(mesh):
    n_row = mesh.shape['sx']
    n_col = mesh.shape['sy']

    def body(forcing, kappa, local_inv, coarse_basis, coarse_counts, coarse_inv):
        size = forcing.shape[0]
        n_rhs = forcing.shape[2]
        edge = math.isqrt(local_inv.shape[1])
        over = (edge - size) // 2
        kmax = coarse_basis.shape[2]
        ktot = coarse_inv.shape[0]
        own = size * size
        count = jnp.broadcast_to(coarse_counts.astype(F32)[:, None], (SUB, LANES))
        kernel, scratch = make_kernel(n_row, n_col, size, over, n_rhs, kmax, ktot)
        vmem = pl.BlockSpec(memory_space=pltpu.VMEM)
        hbm = pl.BlockSpec(memory_space=pl.ANY)
        solved, norms = pl.pallas_call(
            kernel,
            out_shape=(jax.ShapeDtypeStruct((own, n_rhs), F32), jax.ShapeDtypeStruct((ITERS, n_rhs), F32)),
            in_specs=[hbm, vmem, hbm, vmem, vmem, vmem],
            out_specs=(vmem, vmem),
            scratch_shapes=scratch,
            compiler_params=pltpu.CompilerParams(collective_id=0, has_side_effects=True, vmem_limit_bytes=67043328),
        )(forcing.reshape(own, n_rhs), kappa, local_inv.reshape(edge, edge, edge * edge), coarse_basis[0].T, count, coarse_inv)
        return solved.reshape(size, size, n_rhs), norms

    cell_spec = P(('batch', 'sx'), 'sy', None)
    sub_spec = P(('batch', 'sx', 'sy'), None, None)
    return jax.shard_map(body, mesh=mesh, in_specs=(cell_spec, P(('batch', 'sx'), 'sy'), sub_spec, sub_spec, P(('batch', 'sx', 'sy')), P('batch', None)), out_specs=(cell_spec, P('batch', None)), check_vma=False)
```
